32 devices in a mesh: groups: 2 (over x), ep: 16 (over z, y, core).
Axes of the slice: x: 2, y: 2, z: 4, core: 2. Of those that a mesh axis runs over, the one named last changes fastest.
Arguments:
- tokens: bfloat16 [256, 7168], P(('groups', 'ep')), parts along dimension 0, may hold values from -6 to 6
- experts: int32 [256, 8], P(('groups', 'ep')), parts along dimension 0, may hold values from 0 to 15, as said below
- gate_fixed: int32 [256, 8], P(('groups', 'ep')), parts along dimension 0, may hold values from 1 to 65535
- home_slot: int32 [256], P(('groups', 'ep')), parts along dimension 0, may hold values from 0 to 7, as said below
- bias: float32 [16], replicated, may hold values from -0.5 to 0.5
- w_gate: bfloat16 [7168, 32768], P(None, 'ep'), may hold values from -0.0625 to 0.0625
- w_up: bfloat16 [7168, 32768], P(None, 'ep'), may hold values from -0.0625 to 0.0625
- w_down: bfloat16 [32768, 7168], P('ep'), may hold values from -0.125 to 0.125
Outputs:
- moe_out: bfloat16 [256, 7168], P(('groups', 'ep')), parts along dimension 0
- bias_next: float32 [32], P('groups'), parts along dimension 0
The draws below stay inside these ranges and needn't reach their ends.
There are 2 independent parts, one for each index of `groups`. The reference program is written for one: setup_inputs(seed, part) draws one part's arguments, and reference() takes and returns one part's arrays. A program takes and returns all parts, laid end to end along the dimension named above; an argument that names none is the same for every part. Nothing has to cross between parts.
Inputs may be any that keep to these rules, and one draw needn't show every extreme that they name: Each token names 8 different experts; among the tokens of one device no expert is named more than 6 times, and some device reaches that bound. `home_slot`: within each device's block of 8 tokens every value appears exactly once.
All inputs are finite; a program needn't handle non-finite values.
Results may differ from the reference program's by a relative error of at most 0.008.
Values may be sent and summed in bfloat16 or wider, within the bound.
A program may use at most 128 MiB of HBM per device.

```python
import math
import jax
import jax.numpy as jnp
from jax import lax

D = 7168
FF = 2048
TOP = 8
EXPERTS = 16
TOK_DEV = 8
SHARDS = 1
FF_DEV = 2048
TOKENS = 128
CAP = 6
N_EP = 16


def draw_home_slot(key, part):
    block_count = TOKENS // TOK_DEV
    scores = jax.random.randint(key, (block_count, TOK_DEV), 0, 1 << 20, dtype=jnp.int32)
    scores = scores * TOK_DEV + jnp.arange(TOK_DEV, dtype=jnp.int32)[None, :]
    ordering = jnp.argsort(scores, axis=1, stable=True).astype(jnp.int32)
    return ordering.reshape(TOKENS)


def draw_experts(key, part):
    block_count = TOKENS // TOK_DEV
    pair_count = TOK_DEV * TOP
    narrow = min(EXPERTS, max(TOP, -(-pair_count // CAP)))
    base = jax.random.fold_in(key, 17)
    first_key = jax.random.fold_in(base, 1)
    second_key = jax.random.fold_in(base, 2)
    third_key = jax.random.fold_in(base, 3)
    common_scores = jax.random.randint(first_key, (EXPERTS,), 0, 1 << 20, dtype=jnp.int32)
    common_scores = common_scores * EXPERTS + jnp.arange(EXPERTS, dtype=jnp.int32)
    common = jnp.argsort(common_scores, stable=True).astype(jnp.int32)
    block_scores = jax.random.randint(second_key, (block_count, EXPERTS), 0, 1 << 20, dtype=jnp.int32)
    block_scores = block_scores * EXPERTS + jnp.arange(EXPERTS, dtype=jnp.int32)[None, :]
    block_order = jnp.argsort(block_scores, axis=1, stable=True).astype(jnp.int32)
    coin = jax.random.randint(third_key, (block_count,), 0, max(block_count - 1, 1), dtype=jnp.int32)
    concentrated = coin < jnp.arange(block_count, dtype=jnp.int32)
    pair_index = jnp.arange(pair_count, dtype=jnp.int32)
    hot_ids = common[pair_index % narrow]
    spread_index = jnp.broadcast_to((pair_index % EXPERTS)[None, :], (block_count, pair_count))
    spread_ids = jnp.take_along_axis(block_order, spread_index, axis=1)
    chosen = jnp.where(concentrated[:, None], hot_ids[None, :], spread_ids)
    return chosen.reshape(TOKENS, TOP).astype(jnp.int32)


def plant(values, rng, least, high):
    place = [jax.random.randint(jax.random.fold_in(rng, axis), (), 0, length) for axis, length in enumerate(values.shape)]
    longest = values.shape.index(max(values.shape))
    neighbour = place[:longest] + [(place[longest] + 1) % values.shape[longest]] + place[longest + 1:]
    return values.at[tuple(place)].set(least).at[tuple(neighbour)].set(high)


def block_levels(stream_key, shape, cuts, smallest, largest):
    def one(dim, blocks):
        draws = jax.random.uniform(jax.random.fold_in(jax.random.fold_in(stream_key, 6), dim), (blocks,), jnp.float32, smallest / len(cuts), largest / len(cuts))
        return jnp.repeat(jnp.exp(draws), shape[dim] // blocks).reshape((-1,) + (1,) * (len(shape) - dim - 1))

    factor_of = one(*cuts[0])
    for cut in cuts[1:]:
        factor_of = factor_of * one(*cut)
    return factor_of


def normal_values(stream_key, extent, deviation, reach, split=(), kind=jnp.bfloat16):
    factor_of = block_levels(stream_key, extent, split, -0.22, 0.18) if split else 1.0
    result = jax.random.normal(stream_key, extent, jnp.float32) * deviation * factor_of
    return jnp.minimum(jnp.maximum(result, -reach), reach).astype(kind)


def setup_inputs(seed: int = 0, part: int = 0) -> dict:
    key_list = jax.random.split(jax.random.key(seed), 9)
    part_keys = jax.random.split(jax.random.fold_in(key_list[8], part), 9)
    tokens = normal_values(part_keys[0], (TOKENS, D), 1.0, 6.0, ((0, 16),))
    experts = draw_experts(jax.random.fold_in(jax.random.fold_in(key_list[8], part), 71), part)
    gate_fixed = plant(jax.random.randint(part_keys[2], (TOKENS, TOP), 1, 65536), jax.random.fold_in(part_keys[2], 1), 1, 65535).astype(jnp.int32)
    home_slot = draw_home_slot(jax.random.fold_in(jax.random.fold_in(key_list[8], part), 71), part)
    bias = jnp.clip(jax.random.uniform(key_list[4], (EXPERTS,), jnp.float32, -0.5, 0.5), -0.5, 0.5)
    w_gate = normal_values(key_list[5], (D, EXPERTS * FF), D ** -0.5, 0.0625, ((1, 16),))
    w_up = normal_values(key_list[6], (D, EXPERTS * FF), D ** -0.5, 0.0625, ((1, 16),))
    w_down = normal_values(key_list[7], (EXPERTS * FF, D), FF ** -0.5, 0.125, ((0, 16),))
    return dict(tokens=tokens, experts=experts, gate_fixed=gate_fixed, home_slot=home_slot, bias=bias, w_gate=w_gate, w_up=w_up, w_down=w_down)


ROUTED_SCALE = 2.5

def reference(tokens, experts, gate_fixed, home_slot, bias, w_gate, w_up, w_down):
    pair_count = TOK_DEV * TOP
    flat_ids = experts.reshape(N_EP, pair_count)
    hit_table = (flat_ids[:, :, None] == jnp.arange(EXPERTS, dtype=jnp.int32)[None, None, :]).astype(jnp.int32)
    earlier = jnp.cumsum(hit_table, axis=1) - hit_table
    slot_rank = lax.optimization_barrier(jnp.sum(earlier * hit_table, axis=2)).astype(jnp.int32)
    pair_token = jnp.arange(N_EP, dtype=jnp.int32)[:, None] * TOK_DEV + jnp.arange(pair_count, dtype=jnp.int32)[None, :] // TOP
    position = ((jnp.arange(N_EP, dtype=jnp.int32)[:, None] * EXPERTS + flat_ids) * CAP + slot_rank).reshape(-1)
    fixed_gate = gate_fixed.astype(jnp.float32)
    gate_share = ROUTED_SCALE * fixed_gate / lax.optimization_barrier(jnp.sum(fixed_gate, axis=1, keepdims=True))
    source_table = jnp.full((N_EP * EXPERTS * CAP,), -1, jnp.int32).at[position].set(pair_token.reshape(-1))
    source_table = source_table.reshape(N_EP, EXPERTS, CAP)
    share_table = jnp.zeros((N_EP * EXPERTS * CAP,), jnp.float32).at[position].set(gate_share.reshape(-1))
    share_table = share_table.reshape(N_EP, EXPERTS, CAP)

    def one_expert(running, expert_id):
        index_rows = lax.dynamic_index_in_dim(source_table, expert_id, 1, keepdims=False).reshape(-1)
        share_rows = lax.dynamic_index_in_dim(share_table, expert_id, 1, keepdims=False).reshape(-1)
        valid = index_rows >= 0
        safe_rows = jnp.maximum(index_rows, 0)
        row_block = jnp.where(valid[:, None], tokens[safe_rows], jnp.zeros((), jnp.bfloat16))
        first = (expert_id * FF).astype(jnp.int32)
        gate_cols = lax.dynamic_slice_in_dim(w_gate, first, FF, 1)
        up_cols = lax.dynamic_slice_in_dim(w_up, first, FF, 1)
        down_rows = lax.dynamic_slice_in_dim(w_down, first, FF, 0)
        gate_part = jnp.dot(row_block, gate_cols, preferred_element_type=jnp.float32)
        up_part = jnp.dot(row_block, up_cols, preferred_element_type=jnp.float32)
        hidden = (jax.nn.silu(gate_part) * up_part).astype(jnp.bfloat16)
        row_count = hidden.shape[0]
        hidden_groups = hidden.astype(jnp.float32).reshape(row_count, SHARDS, FF_DEV)
        down_groups = down_rows.astype(jnp.float32).reshape(SHARDS, FF_DEV, D)
        partial_value = jnp.einsum('rsf,sfd->rsd', hidden_groups, down_groups).astype(jnp.bfloat16)
        expert_out = lax.optimization_barrier(jnp.sum(partial_value.astype(jnp.float32), axis=1))
        weighted = jnp.where(valid[:, None], expert_out * share_rows[:, None], jnp.zeros((), jnp.float32))
        return (running.at[safe_rows].add(weighted), None)
    start = jnp.zeros((N_EP * TOK_DEV, D), jnp.float32)
    summed, _ = lax.scan(one_expert, start, jnp.arange(EXPERTS, dtype=jnp.int32))
    combined = summed.astype(jnp.bfloat16).reshape(N_EP, TOK_DEV, D)
    block_ids = jnp.broadcast_to(jnp.arange(N_EP, dtype=jnp.int32)[:, None], (N_EP, TOK_DEV))
    placed = jnp.zeros((N_EP, TOK_DEV, D), jnp.bfloat16).at[block_ids, home_slot.reshape(N_EP, TOK_DEV)].set(combined)
    moe_out = placed.reshape(N_EP * TOK_DEV, D)
    load = lax.optimization_barrier(jnp.sum(hit_table, axis=(0, 1))).astype(jnp.float32)
    average = N_EP * TOK_DEV * TOP / EXPERTS
    bias_next = bias + 2.0 / math.sqrt(average) * (average - load)
    return (moe_out, bias_next)
```

```python
import functools
import math

import jax
import jax.numpy as jnp
from jax import lax
from jax.experimental import pallas as pl
from jax.experimental.pallas import tpu as pltpu
from jax.sharding import PartitionSpec as P

ROUTED_SCALE = 2.5


def expert_rows(row_block, w_gate, w_up, w_down):
    gate_part = jnp.dot(row_block, w_gate, preferred_element_type=jnp.float32)
    up_part = jnp.dot(row_block, w_up, preferred_element_type=jnp.float32)
    hidden = (jax.nn.silu(gate_part) * up_part).astype(jnp.bfloat16)
    return jnp.dot(hidden, w_down, preferred_element_type=jnp.float32).astype(jnp.bfloat16)


def general(tokens, experts, gate_fixed, home_slot, bias, w_gate, w_up, w_down):
    tok_rows, model_width = tokens.shape
    top_count = experts.shape[1]
    expert_count = bias.shape[0]
    device_count = lax.axis_size("ep")
    shards = device_count // expert_count
    capacity = max(
        2, min(tok_rows, (3 * tok_rows * top_count + 2 * expert_count - 1) // (2 * expert_count))
    )
    pair_count = tok_rows * top_count
    flat_ids = experts.reshape(pair_count)
    hit_table = (flat_ids[:, None] == jnp.arange(expert_count, dtype=jnp.int32)[None, :]).astype(
        jnp.int32
    )
    earlier = jnp.cumsum(hit_table, axis=0) - hit_table
    slot_rank = jnp.sum(earlier * hit_table, axis=1)
    dest_row = flat_ids * capacity + slot_rank
    pair_source = jnp.arange(pair_count, dtype=jnp.int32) // top_count
    fixed_gate = gate_fixed.astype(jnp.float32)
    gate_share = ROUTED_SCALE * fixed_gate / jnp.sum(fixed_gate, axis=1, keepdims=True)
    outgoing = (
        jnp.zeros((expert_count * capacity, model_width), jnp.bfloat16)
        .at[dest_row]
        .set(tokens[pair_source])
    )
    outgoing = jnp.broadcast_to(
        outgoing.reshape(expert_count, 1, capacity, model_width),
        (expert_count, shards, capacity, model_width),
    )
    outgoing = outgoing.reshape(device_count, capacity, model_width)
    used_slots = jnp.zeros((expert_count * capacity,), jnp.bfloat16).at[dest_row].set(1.0)
    used_slots = jnp.broadcast_to(
        used_slots.reshape(expert_count, 1, capacity), (expert_count, shards, capacity)
    ).reshape(device_count, capacity)
    payload = (outgoing,)
    pieces = (lax.all_to_all(payload[0], "ep", split_axis=0, concat_axis=0, tiled=True),)
    sources, slot_count, _ = pieces[0].shape
    results = expert_rows(
        pieces[0].reshape(sources * slot_count, model_width), w_gate, w_up, w_down
    )
    answer = lax.all_to_all(
        results.reshape(sources, slot_count, model_width),
        "ep",
        split_axis=0,
        concat_axis=0,
        tiled=True,
    )
    landed = (answer,) + tuple(pieces[1:])
    returned = landed[0]
    loads = lax.psum(jnp.sum(hit_table, axis=0), "ep")
    summed = jnp.sum(
        returned.reshape(expert_count, shards, capacity, model_width), axis=1, dtype=jnp.float32
    )
    summed = summed.reshape(expert_count * capacity, model_width)
    picked = summed[dest_row].reshape(tok_rows, top_count, model_width)
    combined = jnp.sum(picked * gate_share[:, :, None], axis=1).astype(jnp.bfloat16)
    placer = (home_slot[None, :] == jnp.arange(tok_rows, dtype=jnp.int32)[:, None]).astype(
        jnp.bfloat16
    )
    placed = jnp.dot(placer, combined, preferred_element_type=jnp.float32).astype(jnp.bfloat16)
    average = tok_rows * device_count * top_count / expert_count
    bias_next = bias + 2.0 / math.sqrt(average) * (average - loads.astype(jnp.float32))
    return (placed, bias_next)


LANES = 128
GAT_COLS = 1024
OUT_COLS = 512
HID_COLS = 1024
SLOTS = 6
LAG_Y, LAG_C = 2, 3
LAG_1, LAG_2, LAG_3 = 2, 6, 12


def flip(z, m, nz):
    bit = 1
    while bit < nz:
        if m & bit:
            z = z + bit - 2 * bit * ((z // bit) % 2)
        bit *= 2
    return z


def moe_kernel(
    nz, experts_total, average,
    tokens_hbm, experts_hbm, gates_hbm, home_hbm, bias_hbm, wg_hbm, wu_hbm, wd_hbm,
    out_ref, bias_out,
    exp_v, gate_v, home_v, bias_v, gath, tab_v, x_v, w_v, acc_v, hid_v, share_v,
    p_v, r1_v, s1_v, r2_v, s2_v, r3_v,
    in_sem, gu_sem, dn_sem, zs, zr, ys, yr, cs, cr,
    s1s, s1r, s2s, s2r, s3s, s3r,
):
    rows, depth = tokens_hbm.shape
    top = exp_v.shape[1]
    ff = hid_v.shape[1]
    chunks = depth // GAT_COLS
    out_count = depth // OUT_COLS
    per_slot = ff // OUT_COLS
    blocks = 4 * nz
    side = 2 * nz
    me = lax.axis_index("ep")
    core = me % 2
    y = (me // 2) % 2
    z = me // 4
    other_core = z * 4 + y * 2 + (1 - core)
    other_y = z * 4 + (1 - y) * 2 + core

    def z_peer(m):
        return flip(z, m, nz) * 4 + y * 2 + core

    def slot_of(zz, yy, cc):
        return (cc * 2 + yy) * nz + zz

    def remote(src, dst, ssem, rsem, peer):
        return pltpu.make_async_remote_copy(
            src_ref=src,
            dst_ref=dst,
            send_sem=ssem,
            recv_sem=rsem,
            device_id={"ep": peer},
            device_id_type=pl.DeviceIdType.MESH,
        )

    mine = slot_of(z, y, core)
    token_copy = pltpu.make_async_copy(tokens_hbm, gath.at[mine], in_sem.at[0])
    small = [
        pltpu.make_async_copy(experts_hbm, exp_v, in_sem.at[1]),
        pltpu.make_async_copy(gates_hbm, gate_v, in_sem.at[2]),
        pltpu.make_async_copy(home_hbm, home_v, in_sem.at[3]),
        pltpu.make_async_copy(bias_hbm, bias_v, in_sem.at[4]),
    ]
    token_copy.start()
    for copy in small:
        copy.start()

    barrier = pltpu.get_barrier_semaphore()
    peers = [other_core, other_y] + [z_peer(m) for m in range(1, nz)]
    for peer in peers:
        pl.semaphore_signal(
            barrier, inc=1, device_id={"ep": peer}, device_id_type=pl.DeviceIdType.MESH
        )

    def gu_copies(g):
        slot = lax.rem(g, SLOTS)
        part = pl.ds(pl.multiple_of(g * GAT_COLS, GAT_COLS), GAT_COLS)
        return [
            pltpu.make_async_copy(w.at[part, :], w_v.at[slot, k], gu_sem.at[g, k])
            for k, w in enumerate((wg_hbm, wu_hbm))
        ]

    def dn_copies(j):
        slot = lax.rem(chunks + lax.div(j, per_slot), SLOTS)
        src = pl.ds(pl.multiple_of(j * OUT_COLS, OUT_COLS), OUT_COLS)
        dst = pl.ds(pl.multiple_of(lax.rem(j, per_slot) * OUT_COLS, OUT_COLS), OUT_COLS)
        return [
            pltpu.make_async_copy(
                wd_hbm.at[pl.ds(k * GAT_COLS, GAT_COLS), src],
                w_v.at[slot, k, :, dst],
                dn_sem.at[j, k],
            )
            for k in range(2)
        ]

    def start_gu(g, carry):
        for copy in gu_copies(g):
            copy.start()
        return carry

    def start_dn(j, carry):
        for copy in dn_copies(j):
            copy.start()
        return carry

    lax.fori_loop(0, min(SLOTS, chunks), start_gu, 0)

    def refill(g):
        @pl.when(g + SLOTS < chunks)
        def _():
            start_gu(g + SLOTS, 0)

        @pl.when(g + SLOTS >= chunks)
        def _():
            first = jnp.minimum((g + SLOTS - chunks) * per_slot, out_count)
            last = jnp.minimum(first + per_slot, out_count)
            lax.fori_loop(first, last, start_dn, 0)

    def cols_of(g):
        return pl.ds(pl.multiple_of(g * GAT_COLS, GAT_COLS), GAT_COLS)

    def send_z(g, m):
        ref = gath.at[mine, :, cols_of(g)]
        return remote(ref, ref, zs.at[g, m], zr.at[g, m], z_peer(m))

    def send_y(g, m):
        ref = gath.at[slot_of(flip(z, m, nz), y, core), :, cols_of(g)]
        return remote(ref, ref, ys.at[g, m], yr.at[g, m], other_y)

    def send_own_y():
        ref = gath.at[mine]
        return remote(ref, ref, ys.at[0, 0], yr.at[0, 0], other_y)

    def send_c(g):
        ref = gath.at[pl.ds(core * side, side), :, cols_of(g)]
        return remote(ref, ref, cs.at[g], cr.at[g], other_core)

    def table_z(m):
        ref = tab_v.at[mine]
        return remote(ref, ref, zs.at[chunks, m], zr.at[chunks, m], z_peer(m))

    def table_y():
        ref = tab_v.at[pl.ds(slot_of(0, y, core), nz)]
        return remote(ref, ref, ys.at[chunks, 0], yr.at[chunks, 0], other_y)

    def table_c():
        ref = tab_v.at[pl.ds(core * side, side)]
        return remote(ref, ref, cs.at[chunks], cr.at[chunks], other_core)

    z_order = list(range(nz - 1, 0, -1))

    token_copy.wait()
    pl.semaphore_wait(barrier, len(peers))

    send_own_y().start()

    def first_sends(g, carry):
        for m in z_order:
            send_z(g, m).start()
        return carry

    lax.fori_loop(0, chunks, first_sends, 0)

    for copy in small:
        copy.wait()
    lane = lax.broadcasted_iota(jnp.int32, (rows, LANES), 1)
    lane_expert = lane % experts_total
    part = lane // experts_total
    gates = gate_v[...].astype(jnp.float32)
    shares = ROUTED_SCALE * gates / jnp.sum(gates, axis=1, keepdims=True)
    ids = exp_v[...]
    table = jnp.zeros((rows, LANES), jnp.float32)
    hits = jnp.zeros((rows, LANES), jnp.float32)
    for k in range(top):
        match = ids[:, k : k + 1] == lane_expert
        table += jnp.where(match, shares[:, k : k + 1], 0.0)
        hits += jnp.where(match, 1.0, 0.0)
    high = table.astype(jnp.bfloat16).astype(jnp.float32)
    rest = table - high
    middle = rest.astype(jnp.bfloat16).astype(jnp.float32)
    low = rest - middle
    packed = jnp.where(
        part == 0,
        hits,
        jnp.where(part == 1, high, jnp.where(part == 2, middle, jnp.where(part == 3, low, 0.0))),
    )
    tab_v[mine] = packed.astype(jnp.bfloat16)
    for m in z_order:
        table_z(m).start()
    acc_v[...] = jnp.zeros_like(acc_v)

    def spread(b, g):
        pair = jnp.concatenate(
            [
                gath[2 * b, :, cols_of(g)].astype(jnp.float32),
                gath[2 * b + 1, :, cols_of(g)].astype(jnp.float32),
            ],
            axis=0,
        )
        x_v[pl.ds(pl.multiple_of(b * 2 * rows, 2 * rows), 2 * rows), :] = pair.astype(jnp.bfloat16)
        return g

    def stage_z(g):
        for m in range(1, nz):
            send_z(g, m).wait_recv()
            send_y(g, m).start()

    def stage_y(g):
        for m in range(1, nz):
            send_y(g, m).wait_recv()
        send_c(g).start()

    def stage_c(g):
        send_c(g).wait_recv()
        lax.fori_loop(0, blocks // 2, spread, g)
        for copy in gu_copies(g):
            copy.wait()

    def products(g, n):
        slot = lax.rem(g, SLOTS)
        cols = pl.ds(pl.multiple_of(n * HID_COLS, HID_COLS), HID_COLS)
        x = x_v[...]
        gate = jnp.dot(x, w_v[slot, 0, :, cols], preferred_element_type=jnp.float32)
        up = jnp.dot(x, w_v[slot, 1, :, cols], preferred_element_type=jnp.float32)
        return acc_v[0, :, cols] + gate, acc_v[1, :, cols] + up, cols

    def gather_step(i, carry):
        @pl.when(i < chunks)
        def _():
            stage_z(i)

        @pl.when(i == 0)
        def _():
            for m in z_order:
                table_z(m).wait_recv()
            table_y().start()

        @pl.when(i == LAG_Y)
        def _():
            send_own_y().wait_recv()
            table_y().wait_recv()
            table_c().start()

        @pl.when((i >= LAG_Y) & (i < chunks + LAG_Y))
        def _():
            stage_y(i - LAG_Y)

        @pl.when(i >= LAG_C)
        def _():
            g = i - LAG_C
            stage_c(g)

            def body(n, carry):
                gate, up, cols = products(g, n)
                acc_v[0, :, cols] = gate
                acc_v[1, :, cols] = up
                return carry

            lax.fori_loop(0, ff // HID_COLS, body, 0)
            refill(g)

        return carry

    lax.fori_loop(0, chunks + LAG_C - 1, gather_step, 0)

    table_c().wait_recv()
    tables = tab_v[...].astype(jnp.float32).reshape(blocks * rows, LANES)
    lane = lax.broadcasted_iota(jnp.int32, (blocks * rows, LANES), 1)
    wanted = (lane % experts_total == me) & (lane // experts_total > 0)
    share = jnp.sum(jnp.where(wanted, tables, 0.0), axis=1, keepdims=True)
    share_v[...] = jnp.broadcast_to(share, share_v.shape)
    load = jnp.sum(tables, axis=0, keepdims=True)[:, :experts_total]
    bias_out[...] = bias_v[...] + 2.0 / math.sqrt(average) * (average - load)

    stage_c(chunks - 1)

    def last_body(n, carry):
        gate, up, cols = products(chunks - 1, n)
        hid_v[:, cols] = (gate / (1.0 + jnp.exp(-gate)) * up).astype(jnp.bfloat16)
        return carry

    lax.fori_loop(0, ff // HID_COLS, last_body, 0)
    refill(chunks - 1)

    def send_1(j):
        return remote(p_v.at[j, 1 - core], r1_v.at[j], s1s.at[j], s1r.at[j], other_core)

    def send_2(j):
        return remote(s1_v.at[j, 1 - y], r2_v.at[j], s2s.at[j], s2r.at[j], other_y)

    def send_3(j, m):
        return remote(
            s2_v.at[j, flip(z, m, nz)], r3_v.at[j, m - 1], s3s.at[j, m], s3r.at[j, m], z_peer(m)
        )

    half = blocks * rows // 2
    quarter = half // 2
    home = home_v[...]
    row_id = lax.broadcasted_iota(jnp.int32, (rows, 1), 0)

    def step(j, carry):
        @pl.when(j < out_count)
        def _():
            for copy in dn_copies(j):
                copy.wait()
            slot = lax.rem(chunks + lax.div(j, per_slot), SLOTS)
            cols = pl.ds(pl.multiple_of(lax.rem(j, per_slot) * OUT_COLS, OUT_COLS), OUT_COLS)
            value = jnp.dot(
                hid_v[:, :GAT_COLS], w_v[slot, 0, :, cols], preferred_element_type=jnp.float32
            )
            value += jnp.dot(
                hid_v[:, GAT_COLS:], w_v[slot, 1, :, cols], preferred_element_type=jnp.float32
            )
            value = (value * share_v[:, :1]).astype(jnp.bfloat16)
            p_v[j, 0] = value[:half]
            p_v[j, 1] = value[half:]
            send_1(j).start()

        @pl.when((j >= LAG_1) & (j < out_count + LAG_1))
        def _():
            i = j - LAG_1
            send_1(i).wait_recv()
            value = p_v[i, core].astype(jnp.float32) + r1_v[i].astype(jnp.float32)
            value = value.astype(jnp.bfloat16)
            s1_v[i, 0] = value[:quarter]
            s1_v[i, 1] = value[quarter:]
            send_2(i).start()

        @pl.when((j >= LAG_2) & (j < out_count + LAG_2))
        def _():
            i = j - LAG_2
            send_2(i).wait_recv()
            value = s1_v[i, y].astype(jnp.float32) + r2_v[i].astype(jnp.float32)
            s2_v[i] = value.reshape(nz, rows, OUT_COLS).astype(jnp.bfloat16)
            for m in z_order:
                send_3(i, m).start()

        @pl.when(j >= LAG_3)
        def _():
            i = j - LAG_3
            value = s2_v[i, z].astype(jnp.float32)
            for m in z_order:
                send_3(i, m).wait_recv()
            for m in z_order:
                value += r3_v[i, m - 1].astype(jnp.float32)
            moved = jnp.zeros_like(value)
            for t in range(rows):
                moved = jnp.where(row_id == home[:, t : t + 1], value[t : t + 1, :], moved)
            cols = pl.ds(pl.multiple_of(i * OUT_COLS, OUT_COLS), OUT_COLS)
            out_ref[:, cols] = moved.astype(jnp.bfloat16)

        return carry

    lax.fori_loop(0, out_count + LAG_3, step, 0)

    send_own_y().wait_send()

    def drain_gather(g, carry):
        for m in range(1, nz):
            send_z(g, m).wait_send()
            send_y(g, m).wait_send()
        send_c(g).wait_send()
        return carry

    lax.fori_loop(0, chunks, drain_gather, 0)
    for m in z_order:
        table_z(m).wait_send()
    table_y().wait_send()
    table_c().wait_send()

    def drain(j, carry):
        send_1(j).wait_send()
        send_2(j).wait_send()
        for m in z_order:
            send_3(j, m).wait_send()
        return carry

    lax.fori_loop(0, out_count, drain, 0)


def fits_kernel(tokens, experts, bias, w_gate, device_count):
    rows, depth = tokens.shape
    ff = w_gate.shape[1]
    nz = device_count // 4
    return (
        device_count == bias.shape[0]
        and device_count == 4 * nz
        and nz & (nz - 1) == 0
        and nz > 1
        and rows == 8
        and 4 * bias.shape[0] <= LANES
        and depth % GAT_COLS == 0
        and depth % OUT_COLS == 0
        and ff == 2 * GAT_COLS
        and ff % HID_COLS == 0
        and ff % OUT_COLS == 0
        and depth // GAT_COLS >= SLOTS
        and -(-depth // ff) <= SLOTS
        and SLOTS * 4 * ff * GAT_COLS
        + 8 * device_count * rows * ff
        + 11 * device_count * rows * depth // 2
        < 66000000
    )


def per_device(tokens, experts, gate_fixed, home_slot, bias, w_gate, w_up, w_down):
    device_count = lax.axis_size("ep")
    if not fits_kernel(tokens, experts, bias, w_gate, device_count):
        return general(tokens, experts, gate_fixed, home_slot, bias, w_gate, w_up, w_down)
    rows, depth = tokens.shape
    top = experts.shape[1]
    ff = w_gate.shape[1]
    expert_count = bias.shape[0]
    nz = device_count // 4
    total = device_count * rows
    chunks = depth // GAT_COLS
    out_count = depth // OUT_COLS
    average = rows * device_count * top / expert_count
    bf16 = jnp.bfloat16
    dma = pltpu.SemaphoreType.DMA
    anywhere = pl.BlockSpec(memory_space=pl.ANY)
    out, bias_next = pl.pallas_call(
        functools.partial(moe_kernel, nz, expert_count, average),
        out_shape=(
            jax.ShapeDtypeStruct((rows, depth), bf16),
            jax.ShapeDtypeStruct((1, expert_count), jnp.float32),
        ),
        in_specs=[anywhere] * 8,
        out_specs=(
            pl.BlockSpec(memory_space=pltpu.VMEM),
            pl.BlockSpec(memory_space=pltpu.VMEM),
        ),
        scratch_shapes=[
            pltpu.VMEM((rows, top), jnp.int32),
            pltpu.VMEM((rows, top), jnp.int32),
            pltpu.VMEM((1, rows), jnp.int32),
            pltpu.VMEM((1, expert_count), jnp.float32),
            pltpu.VMEM((device_count, rows, depth), bf16),
            pltpu.VMEM((device_count, rows, LANES), bf16),
            pltpu.VMEM((total, GAT_COLS), bf16),
            pltpu.VMEM((SLOTS, 2, GAT_COLS, ff), bf16),
            pltpu.VMEM((2, total, ff), jnp.float32),
            pltpu.VMEM((total, ff), bf16),
            pltpu.VMEM((total, LANES), jnp.float32),
            pltpu.VMEM((out_count, 2, total // 2, OUT_COLS), bf16),
            pltpu.VMEM((out_count, total // 2, OUT_COLS), bf16),
            pltpu.VMEM((out_count, 2, total // 4, OUT_COLS), bf16),
            pltpu.VMEM((out_count, total // 4, OUT_COLS), bf16),
            pltpu.VMEM((out_count, nz, rows, OUT_COLS), bf16),
            pltpu.VMEM((out_count, nz - 1, rows, OUT_COLS), bf16),
            dma((5,)),
            dma((chunks, 2)),
            dma((out_count, 2)),
            dma((chunks + 1, nz)),
            dma((chunks + 1, nz)),
            dma((chunks + 1, nz)),
            dma((chunks + 1, nz)),
            dma((chunks + 1,)),
            dma((chunks + 1,)),
            dma((out_count,)),
            dma((out_count,)),
            dma((out_count,)),
            dma((out_count,)),
            dma((out_count, nz)),
            dma((out_count, nz)),
        ],
        compiler_params=pltpu.CompilerParams(
            collective_id=0, has_side_effects=True, vmem_limit_bytes=67043328
        ),
    )(
        tokens,
        experts,
        gate_fixed,
        home_slot.reshape(1, rows),
        bias.reshape(1, expert_count),
        w_gate,
        w_up,
        w_down,
    )
    return out, bias_next.reshape(expert_count)


def solution(mesh):
    placed = (
        P(("groups", "ep"), None),
        P(("groups", "ep"), None),
        P(("groups", "ep"), None),
        P(("groups", "ep")),
        P(),
        P(None, "ep"),
        P(None, "ep"),
        P("ep", None),
    )
    return jax.shard_map(
        per_device,
        mesh=mesh,
        in_specs=placed,
        out_specs=(P(("groups", "ep"), None), P("groups")),
        check_vma=False,
    )
```

```python
import functools
import math

import jax
import jax.numpy as jnp
from jax import lax
from jax.experimental import pallas as pl
from jax.experimental.pallas import tpu as pltpu
from jax.sharding import PartitionSpec as P

ROUTED_SCALE = 2.5


def expert_rows(row_block, w_gate, w_up, w_down):
    gate_part = jnp.dot(row_block, w_gate, preferred_element_type=jnp.float32)
    up_part = jnp.dot(row_block, w_up, preferred_element_type=jnp.float32)
    hidden = (jax.nn.silu(gate_part) * up_part).astype(jnp.bfloat16)
    return jnp.dot(hidden, w_down, preferred_element_type=jnp.float32).astype(jnp.bfloat16)


def general(tokens, experts, gate_fixed, home_slot, bias, w_gate, w_up, w_down):
    tok_rows, model_width = tokens.shape
    top_count = experts.shape[1]
    expert_count = bias.shape[0]
    device_count = lax.axis_size("ep")
    shards = device_count // expert_count
    capacity = max(
        2, min(tok_rows, (3 * tok_rows * top_count + 2 * expert_count - 1) // (2 * expert_count))
    )
    pair_count = tok_rows * top_count
    flat_ids = experts.reshape(pair_count)
    hit_table = (flat_ids[:, None] == jnp.arange(expert_count, dtype=jnp.int32)[None, :]).astype(
        jnp.int32
    )
    earlier = jnp.cumsum(hit_table, axis=0) - hit_table
    slot_rank = jnp.sum(earlier * hit_table, axis=1)
    dest_row = flat_ids * capacity + slot_rank
    pair_source = jnp.arange(pair_count, dtype=jnp.int32) // top_count
    fixed_gate = gate_fixed.astype(jnp.float32)
    gate_share = ROUTED_SCALE * fixed_gate / jnp.sum(fixed_gate, axis=1, keepdims=True)
    outgoing = (
        jnp.zeros((expert_count * capacity, model_width), jnp.bfloat16)
        .at[dest_row]
        .set(tokens[pair_source])
    )
    outgoing = jnp.broadcast_to(
        outgoing.reshape(expert_count, 1, capacity, model_width),
        (expert_count, shards, capacity, model_width),
    )
    outgoing = outgoing.reshape(device_count, capacity, model_width)
    used_slots = jnp.zeros((expert_count * capacity,), jnp.bfloat16).at[dest_row].set(1.0)
    used_slots = jnp.broadcast_to(
        used_slots.reshape(expert_count, 1, capacity), (expert_count, shards, capacity)
    ).reshape(device_count, capacity)
    payload = (outgoing,)
    pieces = (lax.all_to_all(payload[0], "ep", split_axis=0, concat_axis=0, tiled=True),)
    sources, slot_count, _ = pieces[0].shape
    results = expert_rows(
        pieces[0].reshape(sources * slot_count, model_width), w_gate, w_up, w_down
    )
    answer = lax.all_to_all(
        results.reshape(sources, slot_count, model_width),
        "ep",
        split_axis=0,
        concat_axis=0,
        tiled=True,
    )
    landed = (answer,) + tuple(pieces[1:])
    returned = landed[0]
    loads = lax.psum(jnp.sum(hit_table, axis=0), "ep")
    summed = jnp.sum(
        returned.reshape(expert_count, shards, capacity, model_width), axis=1, dtype=jnp.float32
    )
    summed = summed.reshape(expert_count * capacity, model_width)
    picked = summed[dest_row].reshape(tok_rows, top_count, model_width)
    combined = jnp.sum(picked * gate_share[:, :, None], axis=1).astype(jnp.bfloat16)
    placer = (home_slot[None, :] == jnp.arange(tok_rows, dtype=jnp.int32)[:, None]).astype(
        jnp.bfloat16
    )
    placed = jnp.dot(placer, combined, preferred_element_type=jnp.float32).astype(jnp.bfloat16)
    average = tok_rows * device_count * top_count / expert_count
    bias_next = bias + 2.0 / math.sqrt(average) * (average - loads.astype(jnp.float32))
    return (placed, bias_next)


LANES = 128
GAT_COLS = 1024
OUT_COLS = 1024
HID_COLS = 2048
SLOTS = 6
LAG_Y, LAG_C = 2, 3
WINDOW = 4
LAG_1, LAG_2, LAG_3 = 1, 4, 7


def flip(z, m, nz):
    bit = 1
    while bit < nz:
        if m & bit:
            z = z + bit - 2 * bit * ((z // bit) % 2)
        bit *= 2
    return z


def moe_kernel(
    nz, experts_total, average,
    tokens_hbm, experts_hbm, gates_hbm, home_hbm, bias_hbm, wg_hbm, wu_hbm, wd_hbm,
    out_ref, bias_out,
    exp_v, gate_v, home_v, bias_v, gath, tab_v, x_v, w_v, acc_v, hid_v, share_v,
    p_v, r1_v, s1_v, r2_v, s2_v, r3_v,
    in_sem, gu_sem, dn_sem, sent, zr, yr, cr, s1r, s2r, s3r,
):
    rows, depth = tokens_hbm.shape
    top = exp_v.shape[1]
    ff = hid_v.shape[1]
    chunks = depth // GAT_COLS
    out_count = depth // OUT_COLS
    per_slot = ff // OUT_COLS
    blocks = 4 * nz
    side = 2 * nz
    me = lax.axis_index("ep")
    core = me % 2
    y = (me // 2) % 2
    z = me // 4
    other_core = z * 4 + y * 2 + (1 - core)
    other_y = z * 4 + (1 - y) * 2 + core

    def z_peer(m):
        return flip(z, m, nz) * 4 + y * 2 + core

    def slot_of(zz, yy, cc):
        return (cc * 2 + yy) * nz + zz

    def remote(src, dst, ssem, rsem, peer):
        return pltpu.make_async_remote_copy(
            src_ref=src,
            dst_ref=dst,
            send_sem=ssem,
            recv_sem=rsem,
            device_id={"ep": peer},
            device_id_type=pl.DeviceIdType.MESH,
        )

    mine = slot_of(z, y, core)
    token_copy = pltpu.make_async_copy(tokens_hbm, gath.at[mine], in_sem.at[0])
    small = [
        pltpu.make_async_copy(experts_hbm, exp_v, in_sem.at[1]),
        pltpu.make_async_copy(gates_hbm, gate_v, in_sem.at[2]),
        pltpu.make_async_copy(home_hbm, home_v, in_sem.at[3]),
        pltpu.make_async_copy(bias_hbm, bias_v, in_sem.at[4]),
    ]
    token_copy.start()
    for copy in small:
        copy.start()

    barrier = pltpu.get_barrier_semaphore()
    peers = [other_core, other_y] + [z_peer(m) for m in range(1, nz)]
    for peer in peers:
        pl.semaphore_signal(
            barrier, inc=1, device_id={"ep": peer}, device_id_type=pl.DeviceIdType.MESH
        )

    def gu_copies(g):
        slot = lax.rem(g, SLOTS)
        part = pl.ds(pl.multiple_of(g * GAT_COLS, GAT_COLS), GAT_COLS)
        return [
            pltpu.make_async_copy(w.at[part, :], w_v.at[slot, k], gu_sem.at[g])
            for k, w in enumerate((wg_hbm, wu_hbm))
        ]

    def dn_copies(j):
        slot = lax.rem(chunks + lax.div(j, per_slot), SLOTS)
        src = pl.ds(pl.multiple_of(j * OUT_COLS, OUT_COLS), OUT_COLS)
        dst = pl.ds(pl.multiple_of(lax.rem(j, per_slot) * OUT_COLS, OUT_COLS), OUT_COLS)
        return [
            pltpu.make_async_copy(
                wd_hbm.at[pl.ds(k * GAT_COLS, GAT_COLS), src],
                w_v.at[slot, k, :, dst],
                dn_sem.at[j],
            )
            for k in range(2)
        ]

    def gu_wait(g):
        ref = w_v.at[lax.rem(g, SLOTS)]
        pltpu.make_async_copy(ref, ref, gu_sem.at[g]).wait()

    def dn_wait(j):
        slot = lax.rem(chunks + lax.div(j, per_slot), SLOTS)
        cols = pl.ds(pl.multiple_of(lax.rem(j, per_slot) * OUT_COLS, OUT_COLS), OUT_COLS)
        ref = w_v.at[slot, :, :, cols]
        pltpu.make_async_copy(ref, ref, dn_sem.at[j]).wait()

    def start_gu(g, carry):
        for copy in gu_copies(g):
            copy.start()
        return carry

    def start_dn(j, carry):
        for copy in dn_copies(j):
            copy.start()
        return carry

    lax.fori_loop(0, min(SLOTS, chunks), start_gu, 0)

    def refill(g):
        @pl.when(g + SLOTS < chunks)
        def _():
            start_gu(g + SLOTS, 0)

        @pl.when(g + SLOTS >= chunks)
        def _():
            first = jnp.minimum((g + SLOTS - chunks) * per_slot, out_count)
            last = jnp.minimum(first + per_slot, out_count)
            lax.fori_loop(first, last, start_dn, 0)

    def cols_of(g):
        return pl.ds(pl.multiple_of(g * GAT_COLS, GAT_COLS), GAT_COLS)

    def send_z(g, m):
        ref = gath.at[mine, :, cols_of(g)]
        return remote(ref, ref, sent.at[0], zr.at[g], z_peer(m))

    def all_z(g):
        ref = gath.at[pl.ds(0, nz - 1), :, cols_of(g)]
        return remote(ref, ref, sent.at[0], zr.at[g], other_y)

    def send_y(g, m):
        ref = gath.at[slot_of(flip(z, m, nz), y, core), :, cols_of(g)]
        return remote(ref, ref, sent.at[1], yr.at[g], other_y)

    def all_y(g):
        ref = gath.at[pl.ds(0, nz - 1), :, cols_of(g)]
        return remote(ref, ref, sent.at[1], yr.at[g], other_y)

    def send_own_y():
        ref = gath.at[mine]
        return remote(ref, ref, sent.at[1], yr.at[chunks], other_y)

    def send_c(g):
        ref = gath.at[pl.ds(core * side, side), :, cols_of(g)]
        return remote(ref, ref, sent.at[2], cr.at[g], other_core)

    def table_z(m):
        ref = tab_v.at[mine]
        return remote(ref, ref, sent.at[3], zr.at[chunks], z_peer(m))

    def all_table_z():
        ref = tab_v.at[pl.ds(0, nz - 1)]
        return remote(ref, ref, sent.at[3], zr.at[chunks], other_y)

    def table_y():
        ref = tab_v.at[pl.ds(slot_of(0, y, core), nz)]
        return remote(ref, ref, sent.at[4], yr.at[chunks + 1], other_y)

    def table_c():
        ref = tab_v.at[pl.ds(core * side, side)]
        return remote(ref, ref, sent.at[5], cr.at[chunks], other_core)

    z_order = list(range(nz - 1, 0, -1))

    token_copy.wait()
    pl.semaphore_wait(barrier, len(peers))

    send_own_y().start()

    def first_sends(g, carry):
        for m in z_order:
            send_z(g, m).start()
        return carry

    first_sends(0, 0)

    for copy in small:
        copy.wait()
    lane = lax.broadcasted_iota(jnp.int32, (rows, LANES), 1)
    lane_expert = lane % experts_total
    part = lane // experts_total
    gates = gate_v[...].astype(jnp.float32)
    shares = ROUTED_SCALE * gates / jnp.sum(gates, axis=1, keepdims=True)
    ids = exp_v[...]
    table = jnp.zeros((rows, LANES), jnp.float32)
    hits = jnp.zeros((rows, LANES), jnp.float32)
    for k in range(top):
        match = ids[:, k : k + 1] == lane_expert
        table += jnp.where(match, shares[:, k : k + 1], 0.0)
        hits += jnp.where(match, 1.0, 0.0)
    high = table.astype(jnp.bfloat16).astype(jnp.float32)
    rest = table - high
    middle = rest.astype(jnp.bfloat16).astype(jnp.float32)
    low = rest - middle
    packed = jnp.where(
        part == 0,
        hits,
        jnp.where(part == 1, high, jnp.where(part == 2, middle, jnp.where(part == 3, low, 0.0))),
    )
    tab_v[mine] = packed.astype(jnp.bfloat16)
    for m in z_order:
        table_z(m).start()
    lax.fori_loop(1, min(WINDOW, chunks), first_sends, 0)
    acc_v[...] = jnp.zeros_like(acc_v)

    def spread(b, g):
        pair = jnp.concatenate(
            [
                gath[2 * b, :, cols_of(g)].astype(jnp.float32),
                gath[2 * b + 1, :, cols_of(g)].astype(jnp.float32),
            ],
            axis=0,
        )
        x_v[pl.ds(pl.multiple_of(b * 2 * rows, 2 * rows), 2 * rows), :] = pair.astype(jnp.bfloat16)
        return g

    def stage_z(g):
        all_z(g).wait_recv()
        for m in range(1, nz):
            send_y(g, m).start()

        @pl.when(g + WINDOW < chunks)
        def _():
            first_sends(g + WINDOW, 0)

    def stage_y(g):
        all_y(g).wait_recv()
        send_c(g).start()

    def stage_c(g):
        send_c(g).wait_recv()
        lax.fori_loop(0, blocks // 2, spread, g)
        gu_wait(g)

    def products(g, n):
        slot = lax.rem(g, SLOTS)
        cols = pl.ds(pl.multiple_of(n * HID_COLS, HID_COLS), HID_COLS)
        x = x_v[...]
        gate = jnp.dot(x, w_v[slot, 0, :, cols], preferred_element_type=jnp.float32)
        up = jnp.dot(x, w_v[slot, 1, :, cols], preferred_element_type=jnp.float32)
        return acc_v[0, :, cols] + gate, acc_v[1, :, cols] + up, cols

    def gather_step(i, carry):
        @pl.when(i < chunks)
        def _():
            stage_z(i)

        @pl.when(i == LAG_Y)
        def _():
            all_table_z().wait_recv()
            table_y().start()
            send_own_y().wait_recv()

        @pl.when(i == LAG_C + 2)
        def _():
            table_y().wait_recv()
            table_c().start()

        @pl.when((i >= LAG_Y) & (i < chunks + LAG_Y))
        def _():
            stage_y(i - LAG_Y)

        @pl.when(i >= LAG_C)
        def _():
            g = i - LAG_C
            stage_c(g)

            def body(n, carry):
                gate, up, cols = products(g, n)
                acc_v[0, :, cols] = gate
                acc_v[1, :, cols] = up
                return carry

            lax.fori_loop(0, ff // HID_COLS, body, 0)
            refill(g)

        return carry

    lax.fori_loop(0, chunks + LAG_C - 1, gather_step, 0)

    stage_c(chunks - 1)

    def last_body(n, carry):
        gate, up, cols = products(chunks - 1, n)
        hid_v[:, cols] = (gate / (1.0 + jnp.exp(-gate)) * up).astype(jnp.bfloat16)
        return carry

    lax.fori_loop(0, ff // HID_COLS, last_body, 0)
    refill(chunks - 1)

    table_c().wait_recv()
    tables = tab_v[...].astype(jnp.float32).reshape(blocks * rows, LANES)
    lane = lax.broadcasted_iota(jnp.int32, (blocks * rows, LANES), 1)
    wanted = (lane % experts_total == me) & (lane // experts_total > 0)
    share = jnp.sum(jnp.where(wanted, tables, 0.0), axis=1, keepdims=True)
    share_v[...] = jnp.broadcast_to(share, share_v.shape)
    load = jnp.sum(tables, axis=0, keepdims=True)[:, :experts_total]
    bias_out[...] = bias_v[...] + 2.0 / math.sqrt(average) * (average - load)

    def send_1(j):
        return remote(p_v.at[j, 1 - core], r1_v.at[j], sent.at[6], s1r.at[j], other_core)

    def send_2(j):
        return remote(s1_v.at[j, 1 - y], r2_v.at[j], sent.at[7], s2r.at[j], other_y)

    def send_3(j, m):
        return remote(
            s2_v.at[j, flip(z, m, nz)], r3_v.at[j, m - 1], sent.at[8], s3r.at[j], z_peer(m)
        )

    def all_3(j):
        return remote(r3_v.at[j], r3_v.at[j], sent.at[8], s3r.at[j], other_y)

    def all_sent(ref, k):
        remote(ref, ref, sent.at[k], zr.at[0], other_y).wait_send()

    half = blocks * rows // 2
    quarter = half // 2
    home = home_v[...]
    row_id = lax.broadcasted_iota(jnp.int32, (rows, 1), 0)

    def step(j, carry):
        @pl.when(j < out_count)
        def _():
            dn_wait(j)
            slot = lax.rem(chunks + lax.div(j, per_slot), SLOTS)
            cols = pl.ds(pl.multiple_of(lax.rem(j, per_slot) * OUT_COLS, OUT_COLS), OUT_COLS)
            value = jnp.dot(
                hid_v[:, :GAT_COLS], w_v[slot, 0, :, cols], preferred_element_type=jnp.float32
            )
            value += jnp.dot(
                hid_v[:, GAT_COLS:], w_v[slot, 1, :, cols], preferred_element_type=jnp.float32
            )
            value = (value * share_v[:, :1]).astype(jnp.bfloat16)
            p_v[j, 0] = value[:half]
            p_v[j, 1] = value[half:]
            send_1(j).start()

        @pl.when((j >= LAG_1) & (j < out_count + LAG_1))
        def _():
            i = j - LAG_1
            send_1(i).wait_recv()
            value = p_v[i, core].astype(jnp.float32) + r1_v[i].astype(jnp.float32)
            value = value.astype(jnp.bfloat16)
            s1_v[i, 0] = value[:quarter]
            s1_v[i, 1] = value[quarter:]
            send_2(i).start()

        @pl.when((j >= LAG_2) & (j < out_count + LAG_2))
        def _():
            i = j - LAG_2
            send_2(i).wait_recv()
            value = s1_v[i, y].astype(jnp.float32) + r2_v[i].astype(jnp.float32)
            s2_v[i] = value.reshape(nz, rows, OUT_COLS).astype(jnp.bfloat16)
            for m in z_order:
                send_3(i, m).start()

        @pl.when(j == LAG_2 + 1)
        def _():
            for k, ref in enumerate(
                (
                    gath.at[pl.ds(0, nz - 1)],
                    gath.at[pl.ds(0, nz)],
                    gath.at[pl.ds(0, side)],
                    tab_v.at[pl.ds(0, nz - 1)],
                    tab_v.at[pl.ds(0, nz)],
                    tab_v.at[pl.ds(0, side)],
                )
            ):
                all_sent(ref, k)

        @pl.when(j >= LAG_3)
        def _():
            i = j - LAG_3
            value = s2_v[i, z].astype(jnp.float32)
            all_3(i).wait_recv()
            for m in z_order:
                value += r3_v[i, m - 1].astype(jnp.float32)
            moved = jnp.zeros_like(value)
            for t in range(rows):
                moved = jnp.where(row_id == home[:, t : t + 1], value[t : t + 1, :], moved)
            cols = pl.ds(pl.multiple_of(i * OUT_COLS, OUT_COLS), OUT_COLS)
            out_ref[:, cols] = moved.astype(jnp.bfloat16)

        return carry

    lax.fori_loop(0, out_count + LAG_3, step, 0)

    all_sent(p_v.at[:, 0], 6)
    all_sent(s1_v.at[:, 0], 7)
    all_sent(s2_v.at[:, pl.ds(0, nz - 1)], 8)


def hand_over(out_in, bias_in, out_ref, bias_ref):
    out_ref[...] = out_in[...]
    bias_ref[...] = bias_in[...]


def fits_kernel(tokens, experts, bias, w_gate, device_count):
    rows, depth = tokens.shape
    ff = w_gate.shape[1]
    nz = device_count // 4
    return (
        device_count == bias.shape[0]
        and device_count == 4 * nz
        and nz & (nz - 1) == 0
        and nz > 1
        and rows == 8
        and 4 * bias.shape[0] <= LANES
        and depth % GAT_COLS == 0
        and depth % OUT_COLS == 0
        and ff == 2 * GAT_COLS
        and ff % HID_COLS == 0
        and ff % OUT_COLS == 0
        and depth // GAT_COLS >= SLOTS
        and -(-depth // ff) <= SLOTS
        and SLOTS * 4 * ff * GAT_COLS
        + 8 * device_count * rows * ff
        + 11 * device_count * rows * depth // 2
        < 66000000
    )


def per_device(tokens, experts, gate_fixed, home_slot, bias, w_gate, w_up, w_down):
    device_count = lax.axis_size("ep")
    if not fits_kernel(tokens, experts, bias, w_gate, device_count):
        return general(tokens, experts, gate_fixed, home_slot, bias, w_gate, w_up, w_down)
    rows, depth = tokens.shape
    top = experts.shape[1]
    ff = w_gate.shape[1]
    expert_count = bias.shape[0]
    nz = device_count // 4
    total = device_count * rows
    chunks = depth // GAT_COLS
    out_count = depth // OUT_COLS
    average = rows * device_count * top / expert_count
    bf16 = jnp.bfloat16
    dma = pltpu.SemaphoreType.DMA
    anywhere = pl.BlockSpec(memory_space=pl.ANY)
    out, bias_next = pl.pallas_call(
        functools.partial(moe_kernel, nz, expert_count, average),
        out_shape=(
            pltpu.VMEM((rows, depth), bf16),
            pltpu.VMEM((1, expert_count), jnp.float32),
        ),
        in_specs=[anywhere] * 8,
        out_specs=(
            pl.BlockSpec(memory_space=pltpu.VMEM),
            pl.BlockSpec(memory_space=pltpu.VMEM),
        ),
        scratch_shapes=[
            pltpu.VMEM((rows, top), jnp.int32),
            pltpu.VMEM((rows, top), jnp.int32),
            pltpu.VMEM((1, rows), jnp.int32),
            pltpu.VMEM((1, expert_count), jnp.float32),
            pltpu.VMEM((device_count, rows, depth), bf16),
            pltpu.VMEM((device_count, rows, LANES), bf16),
            pltpu.VMEM((total, GAT_COLS), bf16),
            pltpu.VMEM((SLOTS, 2, GAT_COLS, ff), bf16),
            pltpu.VMEM((2, total, ff), jnp.float32),
            pltpu.VMEM((total, ff), bf16),
            pltpu.VMEM((total, LANES), jnp.float32),
            pltpu.VMEM((out_count, 2, total // 2, OUT_COLS), bf16),
            pltpu.VMEM((out_count, total // 2, OUT_COLS), bf16),
            pltpu.VMEM((out_count, 2, total // 4, OUT_COLS), bf16),
            pltpu.VMEM((out_count, total // 4, OUT_COLS), bf16),
            pltpu.VMEM((out_count, nz, rows, OUT_COLS), bf16),
            pltpu.VMEM((out_count, nz - 1, rows, OUT_COLS), bf16),
            dma((5,)),
            dma((chunks,)),
            dma((out_count,)),
            dma((9,)),
            dma((chunks + 1,)),
            dma((chunks + 2,)),
            dma((chunks + 1,)),
            dma((out_count,)),
            dma((out_count,)),
            dma((out_count,)),
        ],
        compiler_params=pltpu.CompilerParams(
            collective_id=0, has_side_effects=True, vmem_limit_bytes=66000000
        ),
    )(
        tokens,
        experts,
        gate_fixed,
        home_slot.reshape(1, rows),
        bias.reshape(1, expert_count),
        w_gate,
        w_up,
        w_down,
    )
    vmem = pl.BlockSpec(memory_space=pltpu.VMEM)
    out, bias_next = pl.pallas_call(
        hand_over,
        out_shape=(
            jax.ShapeDtypeStruct((rows, depth), bf16),
            jax.ShapeDtypeStruct((1, expert_count), jnp.float32),
        ),
        in_specs=[vmem, vmem],
        out_specs=(vmem, vmem),
        compiler_params=pltpu.CompilerParams(vmem_limit_bytes=1000000),
    )(out, bias_next)
    return out, bias_next.reshape(expert_count)


def solution(mesh):
    placed = (
        P(("groups", "ep"), None),
        P(("groups", "ep"), None),
        P(("groups", "ep"), None),
        P(("groups", "ep")),
        P(),
        P(None, "ep"),
        P(None, "ep"),
        P("ep", None),
    )
    return jax.shard_map(
        per_device,
        mesh=mesh,
        in_specs=placed,
        out_specs=(P(("groups", "ep"), None), P("groups")),
        check_vma=False,
    )
```

```python
import functools
import math

import jax
import jax.numpy as jnp
from jax import lax
from jax.experimental import pallas as pl
from jax.experimental.pallas import tpu as pltpu
from jax.sharding import PartitionSpec as P

ROUTED_SCALE = 2.5


def expert_rows(row_block, w_gate, w_up, w_down):
    gate_part = jnp.dot(row_block, w_gate, preferred_element_type=jnp.float32)
    up_part = jnp.dot(row_block, w_up, preferred_element_type=jnp.float32)
    hidden = (jax.nn.silu(gate_part) * up_part).astype(jnp.bfloat16)
    return jnp.dot(hidden, w_down, preferred_element_type=jnp.float32).astype(jnp.bfloat16)


def general(tokens, experts, gate_fixed, home_slot, bias, w_gate, w_up, w_down):
    tok_rows, model_width = tokens.shape
    top_count = experts.shape[1]
    expert_count = bias.shape[0]
    device_count = lax.axis_size("ep")
    shards = device_count // expert_count
    capacity = max(
        2, min(tok_rows, (3 * tok_rows * top_count + 2 * expert_count - 1) // (2 * expert_count))
    )
    pair_count = tok_rows * top_count
    flat_ids = experts.reshape(pair_count)
    hit_table = (flat_ids[:, None] == jnp.arange(expert_count, dtype=jnp.int32)[None, :]).astype(
        jnp.int32
    )
    earlier = jnp.cumsum(hit_table, axis=0) - hit_table
    slot_rank = jnp.sum(earlier * hit_table, axis=1)
    dest_row = flat_ids * capacity + slot_rank
    pair_source = jnp.arange(pair_count, dtype=jnp.int32) // top_count
    fixed_gate = gate_fixed.astype(jnp.float32)
    gate_share = ROUTED_SCALE * fixed_gate / jnp.sum(fixed_gate, axis=1, keepdims=True)
    outgoing = (
        jnp.zeros((expert_count * capacity, model_width), jnp.bfloat16)
        .at[dest_row]
        .set(tokens[pair_source])
    )
    outgoing = jnp.broadcast_to(
        outgoing.reshape(expert_count, 1, capacity, model_width),
        (expert_count, shards, capacity, model_width),
    )
    outgoing = outgoing.reshape(device_count, capacity, model_width)
    used_slots = jnp.zeros((expert_count * capacity,), jnp.bfloat16).at[dest_row].set(1.0)
    used_slots = jnp.broadcast_to(
        used_slots.reshape(expert_count, 1, capacity), (expert_count, shards, capacity)
    ).reshape(device_count, capacity)
    payload = (outgoing,)
    pieces = (lax.all_to_all(payload[0], "ep", split_axis=0, concat_axis=0, tiled=True),)
    sources, slot_count, _ = pieces[0].shape
    results = expert_rows(
        pieces[0].reshape(sources * slot_count, model_width), w_gate, w_up, w_down
    )
    answer = lax.all_to_all(
        results.reshape(sources, slot_count, model_width),
        "ep",
        split_axis=0,
        concat_axis=0,
        tiled=True,
    )
    landed = (answer,) + tuple(pieces[1:])
    returned = landed[0]
    loads = lax.psum(jnp.sum(hit_table, axis=0), "ep")
    summed = jnp.sum(
        returned.reshape(expert_count, shards, capacity, model_width), axis=1, dtype=jnp.float32
    )
    summed = summed.reshape(expert_count * capacity, model_width)
    picked = summed[dest_row].reshape(tok_rows, top_count, model_width)
    combined = jnp.sum(picked * gate_share[:, :, None], axis=1).astype(jnp.bfloat16)
    placer = (home_slot[None, :] == jnp.arange(tok_rows, dtype=jnp.int32)[:, None]).astype(
        jnp.bfloat16
    )
    placed = jnp.dot(placer, combined, preferred_element_type=jnp.float32).astype(jnp.bfloat16)
    average = tok_rows * device_count * top_count / expert_count
    bias_next = bias + 2.0 / math.sqrt(average) * (average - loads.astype(jnp.float32))
    return (placed, bias_next)


LANES = 128
GAT_COLS = 1024
OUT_COLS = 1024
HID_COLS = 2048
SLOTS = 6
LAG_Y, LAG_C = 2, 3
AHEAD_0, AHEAD_1 = 7, 2
LAG_1, LAG_2, LAG_3 = 1, 4, 7


def flip(z, m, nz):
    bit = 1
    while bit < nz:
        if m & bit:
            z = z + bit - 2 * bit * ((z // bit) % 2)
        bit *= 2
    return z


def moe_kernel(
    nz, experts_total, average,
    tokens_hbm, experts_hbm, gates_hbm, home_hbm, bias_hbm, wg_hbm, wu_hbm, wd_hbm,
    out_ref, bias_out,
    exp_v, gate_v, home_v, bias_v, gath, tab_v, x_v, w_v, acc_v, hid_v, share_v,
    p_v, r1_v, s1_v, r2_v, s2_v, r3_v,
    in_sem, gu_sem, dn_sem, sent, zr, yr, cr, s1r, s2r, s3r,
):
    rows, depth = tokens_hbm.shape
    top = exp_v.shape[1]
    ff = hid_v.shape[1]
    chunks = depth // GAT_COLS
    out_count = depth // OUT_COLS
    per_slot = ff // OUT_COLS
    blocks = 4 * nz
    side = 2 * nz
    me = lax.axis_index("ep")
    core = me % 2
    y = (me // 2) % 2
    z = me // 4
    other_core = z * 4 + y * 2 + (1 - core)
    other_y = z * 4 + (1 - y) * 2 + core

    def z_peer(m):
        return flip(z, m, nz) * 4 + y * 2 + core

    def slot_of(zz, yy, cc):
        return (cc * 2 + yy) * nz + zz

    def remote(src, dst, ssem, rsem, peer):
        return pltpu.make_async_remote_copy(
            src_ref=src,
            dst_ref=dst,
            send_sem=ssem,
            recv_sem=rsem,
            device_id={"ep": peer},
            device_id_type=pl.DeviceIdType.MESH,
        )

    mine = slot_of(z, y, core)
    token_copy = pltpu.make_async_copy(tokens_hbm, gath.at[mine], in_sem.at[0])
    small = [
        pltpu.make_async_copy(experts_hbm, exp_v, in_sem.at[1]),
        pltpu.make_async_copy(gates_hbm, gate_v, in_sem.at[2]),
        pltpu.make_async_copy(home_hbm, home_v, in_sem.at[3]),
        pltpu.make_async_copy(bias_hbm, bias_v, in_sem.at[4]),
    ]
    token_copy.start()
    for copy in small:
        copy.start()

    barrier = pltpu.get_barrier_semaphore()
    peers = [other_core, other_y] + [z_peer(m) for m in range(1, nz)]
    for peer in peers:
        pl.semaphore_signal(
            barrier, inc=1, device_id={"ep": peer}, device_id_type=pl.DeviceIdType.MESH
        )

    def gu_copies(g):
        slot = lax.rem(g, SLOTS)
        part = pl.ds(pl.multiple_of(g * GAT_COLS, GAT_COLS), GAT_COLS)
        return [
            pltpu.make_async_copy(w.at[part, :], w_v.at[slot, k], gu_sem.at[g])
            for k, w in enumerate((wg_hbm, wu_hbm))
        ]

    def dn_copies(j):
        slot = lax.rem(chunks + lax.div(j, per_slot), SLOTS)
        src = pl.ds(pl.multiple_of(j * OUT_COLS, OUT_COLS), OUT_COLS)
        dst = pl.ds(pl.multiple_of(lax.rem(j, per_slot) * OUT_COLS, OUT_COLS), OUT_COLS)
        return [
            pltpu.make_async_copy(
                wd_hbm.at[pl.ds(k * GAT_COLS, GAT_COLS), src],
                w_v.at[slot, k, :, dst],
                dn_sem.at[j],
            )
            for k in range(2)
        ]

    def gu_wait(g):
        ref = w_v.at[lax.rem(g, SLOTS)]
        pltpu.make_async_copy(ref, ref, gu_sem.at[g]).wait()

    def dn_wait(j):
        slot = lax.rem(chunks + lax.div(j, per_slot), SLOTS)
        cols = pl.ds(pl.multiple_of(lax.rem(j, per_slot) * OUT_COLS, OUT_COLS), OUT_COLS)
        ref = w_v.at[slot, :, :, cols]
        pltpu.make_async_copy(ref, ref, dn_sem.at[j]).wait()

    def start_gu(g, carry):
        for copy in gu_copies(g):
            copy.start()
        return carry

    def start_dn(j, carry):
        for copy in dn_copies(j):
            copy.start()
        return carry

    lax.fori_loop(0, min(SLOTS, chunks), start_gu, 0)

    def refill(g):
        @pl.when(g + SLOTS < chunks)
        def _():
            start_gu(g + SLOTS, 0)

        @pl.when(g + SLOTS >= chunks)
        def _():
            first = jnp.minimum((g + SLOTS - chunks) * per_slot, out_count)
            last = jnp.minimum(first + per_slot, out_count)
            lax.fori_loop(first, last, start_dn, 0)

    def cols_of(g):
        return pl.ds(pl.multiple_of(g * GAT_COLS, GAT_COLS), GAT_COLS)

    def send_z(g, m):
        ref = gath.at[mine, :, cols_of(g)]
        return remote(ref, ref, sent.at[0], zr.at[g], z_peer(m))

    def all_z(g):
        ref = gath.at[pl.ds(0, nz - 1), :, cols_of(g)]
        return remote(ref, ref, sent.at[0], zr.at[g], other_y)

    def send_y(g, m):
        ref = gath.at[slot_of(flip(z, m, nz), y, core), :, cols_of(g)]
        return remote(ref, ref, sent.at[1], yr.at[g], other_y)

    def all_y(g):
        ref = gath.at[pl.ds(0, nz - 1), :, cols_of(g)]
        return remote(ref, ref, sent.at[1], yr.at[g], other_y)

    def send_own_y():
        ref = gath.at[mine]
        return remote(ref, ref, sent.at[1], yr.at[chunks], other_y)

    def send_c(g):
        ref = gath.at[pl.ds(core * side, side), :, cols_of(g)]
        return remote(ref, ref, sent.at[2], cr.at[g], other_core)

    def table_z(m):
        ref = tab_v.at[mine]
        return remote(ref, ref, sent.at[3], zr.at[chunks], z_peer(m))

    def all_table_z():
        ref = tab_v.at[pl.ds(0, nz - 1)]
        return remote(ref, ref, sent.at[3], zr.at[chunks], other_y)

    def table_y():
        ref = tab_v.at[pl.ds(slot_of(0, y, core), nz)]
        return remote(ref, ref, sent.at[4], yr.at[chunks + 1], other_y)

    def table_c():
        ref = tab_v.at[pl.ds(core * side, side)]
        return remote(ref, ref, sent.at[5], cr.at[chunks], other_core)

    z_order = list(range(nz - 1, 0, -1))

    token_copy.wait()
    pl.semaphore_wait(barrier, len(peers))

    send_own_y().start()

    def first_sends(g, carry):
        for m in z_order:
            send_z(g, m).start()
        return carry

    first_sends(0, 0)

    for copy in small:
        copy.wait()
    lane = lax.broadcasted_iota(jnp.int32, (rows, LANES), 1)
    lane_expert = lane % experts_total
    part = lane // experts_total
    gates = gate_v[...].astype(jnp.float32)
    shares = ROUTED_SCALE * gates / jnp.sum(gates, axis=1, keepdims=True)
    ids = exp_v[...]
    table = jnp.zeros((rows, LANES), jnp.float32)
    hits = jnp.zeros((rows, LANES), jnp.float32)
    for k in range(top):
        match = ids[:, k : k + 1] == lane_expert
        table += jnp.where(match, shares[:, k : k + 1], 0.0)
        hits += jnp.where(match, 1.0, 0.0)
    high = table.astype(jnp.bfloat16).astype(jnp.float32)
    rest = table - high
    middle = rest.astype(jnp.bfloat16).astype(jnp.float32)
    low = rest - middle
    packed = jnp.where(
        part == 0,
        hits,
        jnp.where(part == 1, high, jnp.where(part == 2, middle, jnp.where(part == 3, low, 0.0))),
    )
    tab_v[mine] = packed.astype(jnp.bfloat16)
    for m in z_order:
        table_z(m).start()
    ahead = AHEAD_0 + (AHEAD_1 - AHEAD_0) * core
    lax.fori_loop(1, ahead, first_sends, 0)
    acc_v[...] = jnp.zeros_like(acc_v)

    def spread(b, g):
        pair = jnp.concatenate(
            [
                gath[2 * b, :, cols_of(g)].astype(jnp.float32),
                gath[2 * b + 1, :, cols_of(g)].astype(jnp.float32),
            ],
            axis=0,
        )
        x_v[pl.ds(pl.multiple_of(b * 2 * rows, 2 * rows), 2 * rows), :] = pair.astype(jnp.bfloat16)
        return g

    def stage_z(g):
        all_z(g).wait_recv()
        for m in range(1, nz):
            send_y(g, m).start()

        @pl.when(g + ahead < chunks)
        def _():
            first_sends(g + ahead, 0)

    def stage_y(g):
        all_y(g).wait_recv()
        send_c(g).start()

    def stage_c(g):
        send_c(g).wait_recv()
        lax.fori_loop(0, blocks // 2, spread, g)
        gu_wait(g)

    def products(g, n):
        slot = lax.rem(g, SLOTS)
        cols = pl.ds(pl.multiple_of(n * HID_COLS, HID_COLS), HID_COLS)
        x = x_v[...]
        gate = jnp.dot(x, w_v[slot, 0, :, cols], preferred_element_type=jnp.float32)
        up = jnp.dot(x, w_v[slot, 1, :, cols], preferred_element_type=jnp.float32)
        return acc_v[0, :, cols] + gate, acc_v[1, :, cols] + up, cols

    def gather_step(i, carry):
        @pl.when(i < chunks)
        def _():
            stage_z(i)

        @pl.when(i == LAG_Y)
        def _():
            all_table_z().wait_recv()
            table_y().start()
            send_own_y().wait_recv()

        @pl.when(i == LAG_C + 2)
        def _():
            table_y().wait_recv()
            table_c().start()

        @pl.when((i >= LAG_Y) & (i < chunks + LAG_Y))
        def _():
            stage_y(i - LAG_Y)

        @pl.when(i >= LAG_C)
        def _():
            g = i - LAG_C
            stage_c(g)

            def body(n, carry):
                gate, up, cols = products(g, n)
                acc_v[0, :, cols] = gate
                acc_v[1, :, cols] = up
                return carry

            lax.fori_loop(0, ff // HID_COLS, body, 0)
            refill(g)

        return carry

    lax.fori_loop(0, chunks + LAG_C - 1, gather_step, 0)

    stage_c(chunks - 1)

    def last_body(n, carry):
        gate, up, cols = products(chunks - 1, n)
        hid_v[:, cols] = (gate / (1.0 + jnp.exp(-gate)) * up).astype(jnp.bfloat16)
        return carry

    lax.fori_loop(0, ff // HID_COLS, last_body, 0)
    refill(chunks - 1)

    table_c().wait_recv()
    tables = tab_v[...].astype(jnp.float32).reshape(blocks * rows, LANES)
    lane = lax.broadcasted_iota(jnp.int32, (blocks * rows, LANES), 1)
    wanted = (lane % experts_total == me) & (lane // experts_total > 0)
    share = jnp.sum(jnp.where(wanted, tables, 0.0), axis=1, keepdims=True)
    share_v[...] = jnp.broadcast_to(share, share_v.shape)
    load = jnp.sum(tables, axis=0, keepdims=True)[:, :experts_total]
    bias_out[...] = bias_v[...] + 2.0 / math.sqrt(average) * (average - load)

    def send_1(j):
        return remote(p_v.at[j, 1 - core], r1_v.at[j], sent.at[6], s1r.at[j], other_core)

    def send_2(j):
        return remote(s1_v.at[j, 1 - y], r2_v.at[j], sent.at[7], s2r.at[j], other_y)

    def send_3(j, m):
        return remote(
            s2_v.at[j, flip(z, m, nz)], r3_v.at[j, m - 1], sent.at[8], s3r.at[j], z_peer(m)
        )

    def all_3(j):
        return remote(r3_v.at[j], r3_v.at[j], sent.at[8], s3r.at[j], other_y)

    def all_sent(ref, k):
        remote(ref, ref, sent.at[k], zr.at[0], other_y).wait_send()

    half = blocks * rows // 2
    quarter = half // 2
    home = home_v[...]
    row_id = lax.broadcasted_iota(jnp.int32, (rows, 1), 0)

    def step(j, carry):
        @pl.when(j < out_count)
        def _():
            dn_wait(j)
            slot = lax.rem(chunks + lax.div(j, per_slot), SLOTS)
            cols = pl.ds(pl.multiple_of(lax.rem(j, per_slot) * OUT_COLS, OUT_COLS), OUT_COLS)
            value = jnp.dot(
                hid_v[:, :GAT_COLS], w_v[slot, 0, :, cols], preferred_element_type=jnp.float32
            )
            value += jnp.dot(
                hid_v[:, GAT_COLS:], w_v[slot, 1, :, cols], preferred_element_type=jnp.float32
            )
            value = (value * share_v[:, :1]).astype(jnp.bfloat16)
            p_v[j, 0] = value[:half]
            p_v[j, 1] = value[half:]
            send_1(j).start()

        @pl.when((j >= LAG_1) & (j < out_count + LAG_1))
        def _():
            i = j - LAG_1
            send_1(i).wait_recv()
            value = p_v[i, core].astype(jnp.float32) + r1_v[i].astype(jnp.float32)
            value = value.astype(jnp.bfloat16)
            s1_v[i, 0] = value[:quarter]
            s1_v[i, 1] = value[quarter:]
            send_2(i).start()

        @pl.when((j >= LAG_2) & (j < out_count + LAG_2))
        def _():
            i = j - LAG_2
            send_2(i).wait_recv()
            value = s1_v[i, y].astype(jnp.float32) + r2_v[i].astype(jnp.float32)
            s2_v[i] = value.reshape(nz, rows, OUT_COLS).astype(jnp.bfloat16)
            for m in z_order:
                send_3(i, m).start()

        @pl.when(j == LAG_2 + 1)
        def _():
            for k, ref in enumerate(
                (
                    gath.at[pl.ds(0, nz - 1)],
                    gath.at[pl.ds(0, nz)],
                    gath.at[pl.ds(0, side)],
                    tab_v.at[pl.ds(0, nz - 1)],
                    tab_v.at[pl.ds(0, nz)],
                    tab_v.at[pl.ds(0, side)],
                )
            ):
                all_sent(ref, k)

        @pl.when(j >= LAG_3)
        def _():
            i = j - LAG_3
            value = s2_v[i, z].astype(jnp.float32)
            all_3(i).wait_recv()
            for m in z_order:
                value += r3_v[i, m - 1].astype(jnp.float32)
            moved = jnp.zeros_like(value)
            for t in range(rows):
                moved = jnp.where(row_id == home[:, t : t + 1], value[t : t + 1, :], moved)
            cols = pl.ds(pl.multiple_of(i * OUT_COLS, OUT_COLS), OUT_COLS)
            out_ref[:, cols] = moved.astype(jnp.bfloat16)

        return carry

    lax.fori_loop(0, out_count + LAG_3, step, 0)

    all_sent(p_v.at[:, 0], 6)
    all_sent(s1_v.at[:, 0], 7)
    all_sent(s2_v.at[:, pl.ds(0, nz - 1)], 8)


def hand_over(out_in, bias_in, out_ref, bias_ref):
    out_ref[...] = out_in[...]
    bias_ref[...] = bias_in[...]


def fits_kernel(tokens, experts, bias, w_gate, device_count):
    rows, depth = tokens.shape
    ff = w_gate.shape[1]
    nz = device_count // 4
    return (
        device_count == bias.shape[0]
        and device_count == 4 * nz
        and nz & (nz - 1) == 0
        and nz > 1
        and rows == 8
        and 4 * bias.shape[0] <= LANES
        and depth % GAT_COLS == 0
        and depth % OUT_COLS == 0
        and ff == 2 * GAT_COLS
        and ff % HID_COLS == 0
        and ff % OUT_COLS == 0
        and depth // GAT_COLS >= SLOTS
        and -(-depth // ff) <= SLOTS
        and SLOTS * 4 * ff * GAT_COLS
        + 8 * device_count * rows * ff
        + 11 * device_count * rows * depth // 2
        < 66000000
    )


def per_device(tokens, experts, gate_fixed, home_slot, bias, w_gate, w_up, w_down):
    device_count = lax.axis_size("ep")
    if not fits_kernel(tokens, experts, bias, w_gate, device_count):
        return general(tokens, experts, gate_fixed, home_slot, bias, w_gate, w_up, w_down)
    rows, depth = tokens.shape
    top = experts.shape[1]
    ff = w_gate.shape[1]
    expert_count = bias.shape[0]
    nz = device_count // 4
    total = device_count * rows
    chunks = depth // GAT_COLS
    out_count = depth // OUT_COLS
    average = rows * device_count * top / expert_count
    bf16 = jnp.bfloat16
    dma = pltpu.SemaphoreType.DMA
    anywhere = pl.BlockSpec(memory_space=pl.ANY)
    out, bias_next = pl.pallas_call(
        functools.partial(moe_kernel, nz, expert_count, average),
        out_shape=(
            pltpu.VMEM((rows, depth), bf16),
            pltpu.VMEM((1, expert_count), jnp.float32),
        ),
        in_specs=[anywhere] * 8,
        out_specs=(
            pl.BlockSpec(memory_space=pltpu.VMEM),
            pl.BlockSpec(memory_space=pltpu.VMEM),
        ),
        scratch_shapes=[
            pltpu.VMEM((rows, top), jnp.int32),
            pltpu.VMEM((rows, top), jnp.int32),
            pltpu.VMEM((1, rows), jnp.int32),
            pltpu.VMEM((1, expert_count), jnp.float32),
            pltpu.VMEM((device_count, rows, depth), bf16),
            pltpu.VMEM((device_count, rows, LANES), bf16),
            pltpu.VMEM((total, GAT_COLS), bf16),
            pltpu.VMEM((SLOTS, 2, GAT_COLS, ff), bf16),
            pltpu.VMEM((2, total, ff), jnp.float32),
            pltpu.VMEM((total, ff), bf16),
            pltpu.VMEM((total, LANES), jnp.float32),
            pltpu.VMEM((out_count, 2, total // 2, OUT_COLS), bf16),
            pltpu.VMEM((out_count, total // 2, OUT_COLS), bf16),
            pltpu.VMEM((out_count, 2, total // 4, OUT_COLS), bf16),
            pltpu.VMEM((out_count, total // 4, OUT_COLS), bf16),
            pltpu.VMEM((out_count, nz, rows, OUT_COLS), bf16),
            pltpu.VMEM((out_count, nz - 1, rows, OUT_COLS), bf16),
            dma((5,)),
            dma((chunks,)),
            dma((out_count,)),
            dma((9,)),
            dma((chunks + 1,)),
            dma((chunks + 2,)),
            dma((chunks + 1,)),
            dma((out_count,)),
            dma((out_count,)),
            dma((out_count,)),
        ],
        compiler_params=pltpu.CompilerParams(
            collective_id=0, has_side_effects=True, vmem_limit_bytes=66000000
        ),
    )(
        tokens,
        experts,
        gate_fixed,
        home_slot.reshape(1, rows),
        bias.reshape(1, expert_count),
        w_gate,
        w_up,
        w_down,
    )
    vmem = pl.BlockSpec(memory_space=pltpu.VMEM)
    out, bias_next = pl.pallas_call(
        hand_over,
        out_shape=(
            jax.ShapeDtypeStruct((rows, depth), bf16),
            jax.ShapeDtypeStruct((1, expert_count), jnp.float32),
        ),
        in_specs=[vmem, vmem],
        out_specs=(vmem, vmem),
        compiler_params=pltpu.CompilerParams(vmem_limit_bytes=1000000),
    )(out, bias_next)
    return out, bias_next.reshape(expert_count)


def solution(mesh):
    placed = (
        P(("groups", "ep"), None),
        P(("groups", "ep"), None),
        P(("groups", "ep"), None),
        P(("groups", "ep")),
        P(),
        P(None, "ep"),
        P(None, "ep"),
        P("ep", None),
    )
    return jax.shard_map(
        per_device,
        mesh=mesh,
        in_specs=placed,
        out_specs=(P(("groups", "ep"), None), P("groups")),
        check_vma=False,
    )
```

```python
import functools
import math

import jax
import jax.numpy as jnp
from jax import lax
from jax.experimental import pallas as pl
from jax.experimental.pallas import tpu as pltpu
from jax.sharding import PartitionSpec as P

ROUTED_SCALE = 2.5


def expert_rows(row_block, w_gate, w_up, w_down):
    gate_part = jnp.dot(row_block, w_gate, preferred_element_type=jnp.float32)
    up_part = jnp.dot(row_block, w_up, preferred_element_type=jnp.float32)
    hidden = (jax.nn.silu(gate_part) * up_part).astype(jnp.bfloat16)
    return jnp.dot(hidden, w_down, preferred_element_type=jnp.float32).astype(jnp.bfloat16)


def general(tokens, experts, gate_fixed, home_slot, bias, w_gate, w_up, w_down):
    tok_rows, model_width = tokens.shape
    top_count = experts.shape[1]
    expert_count = bias.shape[0]
    device_count = lax.axis_size("ep")
    shards = device_count // expert_count
    capacity = max(
        2, min(tok_rows, (3 * tok_rows * top_count + 2 * expert_count - 1) // (2 * expert_count))
    )
    pair_count = tok_rows * top_count
    flat_ids = experts.reshape(pair_count)
    hit_table = (flat_ids[:, None] == jnp.arange(expert_count, dtype=jnp.int32)[None, :]).astype(
        jnp.int32
    )
    earlier = jnp.cumsum(hit_table, axis=0) - hit_table
    slot_rank = jnp.sum(earlier * hit_table, axis=1)
    dest_row = flat_ids * capacity + slot_rank
    pair_source = jnp.arange(pair_count, dtype=jnp.int32) // top_count
    fixed_gate = gate_fixed.astype(jnp.float32)
    gate_share = ROUTED_SCALE * fixed_gate / jnp.sum(fixed_gate, axis=1, keepdims=True)
    outgoing = (
        jnp.zeros((expert_count * capacity, model_width), jnp.bfloat16)
        .at[dest_row]
        .set(tokens[pair_source])
    )
    outgoing = jnp.broadcast_to(
        outgoing.reshape(expert_count, 1, capacity, model_width),
        (expert_count, shards, capacity, model_width),
    )
    outgoing = outgoing.reshape(device_count, capacity, model_width)
    used_slots = jnp.zeros((expert_count * capacity,), jnp.bfloat16).at[dest_row].set(1.0)
    used_slots = jnp.broadcast_to(
        used_slots.reshape(expert_count, 1, capacity), (expert_count, shards, capacity)
    ).reshape(device_count, capacity)
    payload = (outgoing,)
    pieces = (lax.all_to_all(payload[0], "ep", split_axis=0, concat_axis=0, tiled=True),)
    sources, slot_count, _ = pieces[0].shape
    results = expert_rows(
        pieces[0].reshape(sources * slot_count, model_width), w_gate, w_up, w_down
    )
    answer = lax.all_to_all(
        results.reshape(sources, slot_count, model_width),
        "ep",
        split_axis=0,
        concat_axis=0,
        tiled=True,
    )
    landed = (answer,) + tuple(pieces[1:])
    returned = landed[0]
    loads = lax.psum(jnp.sum(hit_table, axis=0), "ep")
    summed = jnp.sum(
        returned.reshape(expert_count, shards, capacity, model_width), axis=1, dtype=jnp.float32
    )
    summed = summed.reshape(expert_count * capacity, model_width)
    picked = summed[dest_row].reshape(tok_rows, top_count, model_width)
    combined = jnp.sum(picked * gate_share[:, :, None], axis=1).astype(jnp.bfloat16)
    placer = (home_slot[None, :] == jnp.arange(tok_rows, dtype=jnp.int32)[:, None]).astype(
        jnp.bfloat16
    )
    placed = jnp.dot(placer, combined, preferred_element_type=jnp.float32).astype(jnp.bfloat16)
    average = tok_rows * device_count * top_count / expert_count
    bias_next = bias + 2.0 / math.sqrt(average) * (average - loads.astype(jnp.float32))
    return (placed, bias_next)


LANES = 128
GAT_COLS = 1024
OUT_COLS = 512
HID_COLS = 2048
SLOTS = 6
LAG_Y, LAG_C = 2, 3
AHEAD_0, AHEAD_1 = 7, 2
LAG_1, LAG_2, LAG_3 = 2, 7, 13


def flip(z, m, nz):
    bit = 1
    while bit < nz:
        if m & bit:
            z = z + bit - 2 * bit * ((z // bit) % 2)
        bit *= 2
    return z


def moe_kernel(
    nz, experts_total, average,
    tokens_hbm, experts_hbm, gates_hbm, home_hbm, bias_hbm, wg_hbm, wu_hbm, wd_hbm,
    out_ref, bias_out,
    exp_v, gate_v, home_v, bias_v, gath, tab_v, x_v, w_v, acc_v, hid_v, share_v,
    p_v, r1_v, s1_v, r2_v, s2_v, r3_v,
    in_sem, gu_sem, dn_sem, sent, zr, yr, cr, s1r, s2r, s3r,
):
    rows, depth = tokens_hbm.shape
    top = exp_v.shape[1]
    ff = hid_v.shape[1]
    chunks = depth // GAT_COLS
    out_count = depth // OUT_COLS
    per_slot = ff // OUT_COLS
    blocks = 4 * nz
    side = 2 * nz
    me = lax.axis_index("ep")
    core = me % 2
    y = (me // 2) % 2
    z = me // 4
    other_core = z * 4 + y * 2 + (1 - core)
    other_y = z * 4 + (1 - y) * 2 + core

    def z_peer(m):
        return flip(z, m, nz) * 4 + y * 2 + core

    def slot_of(zz, yy, cc):
        return (cc * 2 + yy) * nz + zz

    def remote(src, dst, ssem, rsem, peer):
        return pltpu.make_async_remote_copy(
            src_ref=src,
            dst_ref=dst,
            send_sem=ssem,
            recv_sem=rsem,
            device_id={"ep": peer},
            device_id_type=pl.DeviceIdType.MESH,
        )

    mine = slot_of(z, y, core)
    token_copy = pltpu.make_async_copy(tokens_hbm, gath.at[mine], in_sem.at[0])
    small = [
        pltpu.make_async_copy(experts_hbm, exp_v, in_sem.at[1]),
        pltpu.make_async_copy(gates_hbm, gate_v, in_sem.at[2]),
        pltpu.make_async_copy(home_hbm, home_v, in_sem.at[3]),
        pltpu.make_async_copy(bias_hbm, bias_v, in_sem.at[4]),
    ]
    token_copy.start()
    for copy in small:
        copy.start()

    barrier = pltpu.get_barrier_semaphore()
    peers = [other_core, other_y] + [z_peer(m) for m in range(1, nz)]
    for peer in peers:
        pl.semaphore_signal(
            barrier, inc=1, device_id={"ep": peer}, device_id_type=pl.DeviceIdType.MESH
        )

    def gu_copies(g):
        slot = lax.rem(g, SLOTS)
        part = pl.ds(pl.multiple_of(g * GAT_COLS, GAT_COLS), GAT_COLS)
        return [
            pltpu.make_async_copy(w.at[part, :], w_v.at[slot, k], gu_sem.at[g])
            for k, w in enumerate((wg_hbm, wu_hbm))
        ]

    def dn_copies(j):
        slot = lax.rem(chunks + lax.div(j, per_slot), SLOTS)
        src = pl.ds(pl.multiple_of(j * OUT_COLS, OUT_COLS), OUT_COLS)
        dst = pl.ds(pl.multiple_of(lax.rem(j, per_slot) * OUT_COLS, OUT_COLS), OUT_COLS)
        return [
            pltpu.make_async_copy(
                wd_hbm.at[pl.ds(k * GAT_COLS, GAT_COLS), src],
                w_v.at[slot, k, :, dst],
                dn_sem.at[j],
            )
            for k in range(2)
        ]

    def gu_wait(g):
        ref = w_v.at[lax.rem(g, SLOTS)]
        pltpu.make_async_copy(ref, ref, gu_sem.at[g]).wait()

    def dn_wait(j):
        slot = lax.rem(chunks + lax.div(j, per_slot), SLOTS)
        cols = pl.ds(pl.multiple_of(lax.rem(j, per_slot) * OUT_COLS, OUT_COLS), OUT_COLS)
        ref = w_v.at[slot, :, :, cols]
        pltpu.make_async_copy(ref, ref, dn_sem.at[j]).wait()

    def start_gu(g, carry):
        for copy in gu_copies(g):
            copy.start()
        return carry

    def start_dn(j, carry):
        for copy in dn_copies(j):
            copy.start()
        return carry

    lax.fori_loop(0, min(SLOTS, chunks), start_gu, 0)

    def refill(g):
        @pl.when(g + SLOTS < chunks)
        def _():
            start_gu(g + SLOTS, 0)

        @pl.when(g + SLOTS >= chunks)
        def _():
            first = jnp.minimum((g + SLOTS - chunks) * per_slot, out_count)
            last = jnp.minimum(first + per_slot, out_count)
            lax.fori_loop(first, last, start_dn, 0)

    def cols_of(g):
        return pl.ds(pl.multiple_of(g * GAT_COLS, GAT_COLS), GAT_COLS)

    def send_z(g, m):
        ref = gath.at[mine, :, cols_of(g)]
        return remote(ref, ref, sent.at[0], zr.at[g], z_peer(m))

    def all_z(g):
        ref = gath.at[pl.ds(0, nz - 1), :, cols_of(g)]
        return remote(ref, ref, sent.at[0], zr.at[g], other_y)

    def send_y(g, m):
        ref = gath.at[slot_of(flip(z, m, nz), y, core), :, cols_of(g)]
        return remote(ref, ref, sent.at[0], yr.at[g], other_y)

    def all_y(g):
        ref = gath.at[pl.ds(0, nz - 1), :, cols_of(g)]
        return remote(ref, ref, sent.at[0], yr.at[g], other_y)

    def send_own_y():
        ref = gath.at[mine]
        return remote(ref, ref, sent.at[0], yr.at[chunks], other_y)

    def send_c(g):
        ref = gath.at[pl.ds(core * side, side), :, cols_of(g)]
        return remote(ref, ref, sent.at[0], cr.at[g], other_core)

    def table_z(m):
        ref = tab_v.at[mine]
        return remote(ref, ref, sent.at[1], zr.at[chunks], z_peer(m))

    def all_table_z():
        ref = tab_v.at[pl.ds(0, nz - 1)]
        return remote(ref, ref, sent.at[1], zr.at[chunks], other_y)

    def table_y():
        ref = tab_v.at[pl.ds(slot_of(0, y, core), nz)]
        return remote(ref, ref, sent.at[1], yr.at[chunks + 1], other_y)

    def table_c():
        ref = tab_v.at[pl.ds(core * side, side)]
        return remote(ref, ref, sent.at[1], cr.at[chunks], other_core)

    z_order = list(range(nz - 1, 0, -1))

    token_copy.wait()
    pl.semaphore_wait(barrier, len(peers))

    send_own_y().start()

    def first_sends(g, carry):
        for m in z_order:
            send_z(g, m).start()
        return carry

    first_sends(0, 0)

    for copy in small:
        copy.wait()
    lane = lax.broadcasted_iota(jnp.int32, (rows, LANES), 1)
    lane_expert = lane % experts_total
    part = lane // experts_total
    gates = gate_v[...].astype(jnp.float32)
    shares = ROUTED_SCALE * gates / jnp.sum(gates, axis=1, keepdims=True)
    ids = exp_v[...]
    table = jnp.zeros((rows, LANES), jnp.float32)
    hits = jnp.zeros((rows, LANES), jnp.float32)
    for k in range(top):
        match = ids[:, k : k + 1] == lane_expert
        table += jnp.where(match, shares[:, k : k + 1], 0.0)
        hits += jnp.where(match, 1.0, 0.0)
    high = table.astype(jnp.bfloat16).astype(jnp.float32)
    rest = table - high
    middle = rest.astype(jnp.bfloat16).astype(jnp.float32)
    low = rest - middle
    packed = jnp.where(
        part == 0,
        hits,
        jnp.where(part == 1, high, jnp.where(part == 2, middle, jnp.where(part == 3, low, 0.0))),
    )
    tab_v[mine] = packed.astype(jnp.bfloat16)
    for m in z_order:
        table_z(m).start()
    ahead = AHEAD_0 + (AHEAD_1 - AHEAD_0) * core
    lax.fori_loop(1, ahead, first_sends, 0)
    acc_v[...] = jnp.zeros_like(acc_v)

    def spread(b, g):
        pair = jnp.concatenate(
            [
                gath[2 * b, :, cols_of(g)].astype(jnp.float32),
                gath[2 * b + 1, :, cols_of(g)].astype(jnp.float32),
            ],
            axis=0,
        )
        x_v[pl.ds(pl.multiple_of(b * 2 * rows, 2 * rows), 2 * rows), :] = pair.astype(jnp.bfloat16)
        return g

    def stage_z(g):
        all_z(g).wait_recv()
        for m in range(1, nz):
            send_y(g, m).start()

        @pl.when(g + ahead < chunks)
        def _():
            first_sends(g + ahead, 0)

    def stage_y(g):
        all_y(g).wait_recv()
        send_c(g).start()

    def stage_c(g):
        send_c(g).wait_recv()
        lax.fori_loop(0, blocks // 2, spread, g)
        gu_wait(g)

    def products(g, n):
        slot = lax.rem(g, SLOTS)
        cols = pl.ds(pl.multiple_of(n * HID_COLS, HID_COLS), HID_COLS)
        x = x_v[...]
        gate = jnp.dot(x, w_v[slot, 0, :, cols], preferred_element_type=jnp.float32)
        up = jnp.dot(x, w_v[slot, 1, :, cols], preferred_element_type=jnp.float32)
        return acc_v[0, :, cols] + gate, acc_v[1, :, cols] + up, cols

    def gather_step(i, carry):
        @pl.when(i < chunks)
        def _():
            stage_z(i)

        @pl.when(i == LAG_Y)
        def _():
            all_table_z().wait_recv()
            table_y().start()
            send_own_y().wait_recv()

        @pl.when(i == LAG_C + 2)
        def _():
            table_y().wait_recv()
            table_c().start()

        @pl.when((i >= LAG_Y) & (i < chunks + LAG_Y))
        def _():
            stage_y(i - LAG_Y)

        @pl.when(i >= LAG_C)
        def _():
            g = i - LAG_C
            stage_c(g)

            def body(n, carry):
                gate, up, cols = products(g, n)
                acc_v[0, :, cols] = gate
                acc_v[1, :, cols] = up
                return carry

            lax.fori_loop(0, ff // HID_COLS, body, 0)
            refill(g)

        return carry

    lax.fori_loop(0, chunks + LAG_C - 1, gather_step, 0)

    stage_c(chunks - 1)

    def last_body(n, carry):
        gate, up, cols = products(chunks - 1, n)
        hid_v[:, cols] = (gate / (1.0 + jnp.exp(-gate)) * up).astype(jnp.bfloat16)
        return carry

    lax.fori_loop(0, ff // HID_COLS, last_body, 0)
    refill(chunks - 1)

    table_c().wait_recv()
    tables = tab_v[...].astype(jnp.float32).reshape(blocks * rows, LANES)
    lane = lax.broadcasted_iota(jnp.int32, (blocks * rows, LANES), 1)
    wanted = (lane % experts_total == me) & (lane // experts_total > 0)
    share = jnp.sum(jnp.where(wanted, tables, 0.0), axis=1, keepdims=True)
    share_v[...] = jnp.broadcast_to(share, share_v.shape)
    load = jnp.sum(tables, axis=0, keepdims=True)[:, :experts_total]
    bias_out[...] = bias_v[...] + 2.0 / math.sqrt(average) * (average - load)

    def send_1(j):
        return remote(p_v.at[j, 1 - core], r1_v.at[j], sent.at[2], s1r.at[j], other_core)

    def send_2(j):
        return remote(s1_v.at[j, 1 - y], r2_v.at[j], sent.at[3], s2r.at[j], other_y)

    def send_3(j, m):
        return remote(
            s2_v.at[j, flip(z, m, nz)], r3_v.at[j, m - 1], sent.at[4], s3r.at[j], z_peer(m)
        )

    def all_3(j):
        return remote(r3_v.at[j], r3_v.at[j], sent.at[4], s3r.at[j], other_y)

    def all_sent(ref, k):
        remote(ref, ref, sent.at[k], zr.at[0], other_y).wait_send()

    half = blocks * rows // 2
    quarter = half // 2
    home = home_v[...]
    row_id = lax.broadcasted_iota(jnp.int32, (rows, 1), 0)

    def step(j, carry):
        @pl.when(j < out_count)
        def _():
            dn_wait(j)
            slot = lax.rem(chunks + lax.div(j, per_slot), SLOTS)
            cols = pl.ds(pl.multiple_of(lax.rem(j, per_slot) * OUT_COLS, OUT_COLS), OUT_COLS)
            value = jnp.dot(
                hid_v[:, :GAT_COLS], w_v[slot, 0, :, cols], preferred_element_type=jnp.float32
            )
            value += jnp.dot(
                hid_v[:, GAT_COLS:], w_v[slot, 1, :, cols], preferred_element_type=jnp.float32
            )
            value = (value * share_v[:, :1]).astype(jnp.bfloat16)
            p_v[j, 0] = value[:half]
            p_v[j, 1] = value[half:]
            send_1(j).start()

        @pl.when((j >= LAG_1) & (j < out_count + LAG_1))
        def _():
            i = j - LAG_1
            send_1(i).wait_recv()
            value = p_v[i, core].astype(jnp.float32) + r1_v[i].astype(jnp.float32)
            value = value.astype(jnp.bfloat16)
            s1_v[i, 0] = value[:quarter]
            s1_v[i, 1] = value[quarter:]
            send_2(i).start()

        @pl.when((j >= LAG_2) & (j < out_count + LAG_2))
        def _():
            i = j - LAG_2
            send_2(i).wait_recv()
            value = s1_v[i, y].astype(jnp.float32) + r2_v[i].astype(jnp.float32)
            s2_v[i] = value.reshape(nz, rows, OUT_COLS).astype(jnp.bfloat16)
            for m in z_order:
                send_3(i, m).start()

        @pl.when(j == LAG_2 + 1)
        def _():
            all_sent(gath.at[pl.ds(0, blocks - 1)], 0)
            all_sent(tab_v.at[pl.ds(0, blocks - 1)], 1)

        @pl.when(j >= LAG_3)
        def _():
            i = j - LAG_3
            value = s2_v[i, z].astype(jnp.float32)
            all_3(i).wait_recv()
            for m in z_order:
                value += r3_v[i, m - 1].astype(jnp.float32)
            moved = jnp.zeros_like(value)
            for t in range(rows):
                moved = jnp.where(row_id == home[:, t : t + 1], value[t : t + 1, :], moved)
            cols = pl.ds(pl.multiple_of(i * OUT_COLS, OUT_COLS), OUT_COLS)
            out_ref[:, cols] = moved.astype(jnp.bfloat16)

        return carry

    lax.fori_loop(0, out_count + LAG_3, step, 0)

    all_sent(p_v.at[:, 0], 2)
    all_sent(s1_v.at[:, 0], 3)
    all_sent(s2_v.at[:, pl.ds(0, nz - 1)], 4)


def hand_over(out_in, bias_in, out_ref, bias_ref, sem):
    copies = [
        pltpu.make_async_copy(out_in, out_ref, sem.at[0]),
        pltpu.make_async_copy(bias_in, bias_ref, sem.at[1]),
    ]
    for copy in copies:
        copy.start()
    for copy in copies:
        copy.wait()


def fits_kernel(tokens, experts, bias, w_gate, device_count):
    rows, depth = tokens.shape
    ff = w_gate.shape[1]
    nz = device_count // 4
    return (
        device_count == bias.shape[0]
        and device_count == 4 * nz
        and nz & (nz - 1) == 0
        and nz > 1
        and rows == 8
        and 4 * bias.shape[0] <= LANES
        and depth % GAT_COLS == 0
        and depth % OUT_COLS == 0
        and ff == 2 * GAT_COLS
        and ff % HID_COLS == 0
        and ff % OUT_COLS == 0
        and depth // GAT_COLS >= SLOTS
        and -(-depth // ff) <= SLOTS
        and SLOTS * 4 * ff * GAT_COLS
        + 8 * device_count * rows * ff
        + 11 * device_count * rows * depth // 2
        < 66000000
    )


def per_device(tokens, experts, gate_fixed, home_slot, bias, w_gate, w_up, w_down):
    device_count = lax.axis_size("ep")
    if not fits_kernel(tokens, experts, bias, w_gate, device_count):
        return general(tokens, experts, gate_fixed, home_slot, bias, w_gate, w_up, w_down)
    rows, depth = tokens.shape
    top = experts.shape[1]
    ff = w_gate.shape[1]
    expert_count = bias.shape[0]
    nz = device_count // 4
    total = device_count * rows
    chunks = depth // GAT_COLS
    out_count = depth // OUT_COLS
    average = rows * device_count * top / expert_count
    bf16 = jnp.bfloat16
    dma = pltpu.SemaphoreType.DMA
    anywhere = pl.BlockSpec(memory_space=pl.ANY)
    out, bias_next = pl.pallas_call(
        functools.partial(moe_kernel, nz, expert_count, average),
        out_shape=(
            pltpu.VMEM((rows, depth), bf16),
            pltpu.VMEM((1, expert_count), jnp.float32),
        ),
        in_specs=[anywhere] * 8,
        out_specs=(
            pl.BlockSpec(memory_space=pltpu.VMEM),
            pl.BlockSpec(memory_space=pltpu.VMEM),
        ),
        scratch_shapes=[
            pltpu.VMEM((rows, top), jnp.int32),
            pltpu.VMEM((rows, top), jnp.int32),
            pltpu.VMEM((1, rows), jnp.int32),
            pltpu.VMEM((1, expert_count), jnp.float32),
            pltpu.VMEM((device_count, rows, depth), bf16),
            pltpu.VMEM((device_count, rows, LANES), bf16),
            pltpu.VMEM((total, GAT_COLS), bf16),
            pltpu.VMEM((SLOTS, 2, GAT_COLS, ff), bf16),
            pltpu.VMEM((2, total, ff), jnp.float32),
            pltpu.VMEM((total, ff), bf16),
            pltpu.VMEM((total, LANES), jnp.float32),
            pltpu.VMEM((out_count, 2, total // 2, OUT_COLS), bf16),
            pltpu.VMEM((out_count, total // 2, OUT_COLS), bf16),
            pltpu.VMEM((out_count, 2, total // 4, OUT_COLS), bf16),
            pltpu.VMEM((out_count, total // 4, OUT_COLS), bf16),
            pltpu.VMEM((out_count, nz, rows, OUT_COLS), bf16),
            pltpu.VMEM((out_count, nz - 1, rows, OUT_COLS), bf16),
            dma((5,)),
            dma((chunks,)),
            dma((out_count,)),
            dma((5,)),
            dma((chunks + 1,)),
            dma((chunks + 2,)),
            dma((chunks + 1,)),
            dma((out_count,)),
            dma((out_count,)),
            dma((out_count,)),
        ],
        compiler_params=pltpu.CompilerParams(
            collective_id=0, has_side_effects=True, vmem_limit_bytes=66000000
        ),
    )(
        tokens,
        experts,
        gate_fixed,
        home_slot.reshape(1, rows),
        bias.reshape(1, expert_count),
        w_gate,
        w_up,
        w_down,
    )
    vmem = pl.BlockSpec(memory_space=pltpu.VMEM)
    out, bias_next = pl.pallas_call(
        hand_over,
        out_shape=(
            jax.ShapeDtypeStruct((rows, depth), bf16),
            jax.ShapeDtypeStruct((1, expert_count), jnp.float32),
        ),
        in_specs=[vmem, vmem],
        out_specs=(anywhere, anywhere),
        scratch_shapes=[dma((2,))],
        compiler_params=pltpu.CompilerParams(vmem_limit_bytes=1000000),
    )(out, bias_next)
    return out, bias_next.reshape(expert_count)


def solution(mesh):
    placed = (
        P(("groups", "ep"), None),
        P(("groups", "ep"), None),
        P(("groups", "ep"), None),
        P(("groups", "ep")),
        P(),
        P(None, "ep"),
        P(None, "ep"),
        P("ep", None),
    )
    return jax.shard_map(
        per_device,
        mesh=mesh,
        in_specs=placed,
        out_specs=(P(("groups", "ep"), None), P("groups")),
        check_vma=False,
    )
```
